32 devices in a mesh: groups: 2 (over x), sp: 8 (over z, y), fsdp: 2 (over core).
Axes of the slice: x: 2, y: 2, z: 4, core: 2. Of those that a mesh axis runs over, the one named last changes fastest.
Arguments:
- policy_hidden: bfloat16 [4, 256, 4096], P(('groups', 'fsdp'), 'sp'), parts along dimension 0, may hold values from -6 to 6
- policy_queries: bfloat16 [4, 256, 1024], P(('groups', 'fsdp'), 'sp'), parts along dimension 0, may hold values from -512 to 512
- policy_documents: int32 [4, 256], P(('groups', 'fsdp'), 'sp'), parts along dimension 0, may hold values from 0 to 31, never falling along the last dimension, each value on 1 to 128 neighbouring positions
- policy_gain: bfloat16 [4096], P(('sp', 'fsdp')), may hold values from 0.099609375 to 1.8984375
- policy_key_weight: bfloat16 [4096, 512], P(('sp', 'fsdp')), may hold values from -0.09375 to 0.09375
- policy_value_weight: bfloat16 [4096, 512], P(('sp', 'fsdp')), may hold values from -0.09375 to 0.09375
- frozen_hidden: bfloat16 [4, 256, 4096], P(('groups', 'fsdp'), 'sp'), parts along dimension 0, may hold values from -6 to 6
- frozen_queries: bfloat16 [4, 256, 1024], P(('groups', 'fsdp'), 'sp'), parts along dimension 0, may hold values from -512 to 512
- frozen_documents: int32 [4, 256], P(('groups', 'fsdp'), 'sp'), parts along dimension 0, may hold values from 0 to 31, never falling along the last dimension, each value on 1 to 128 neighbouring positions
- frozen_gain: bfloat16 [4096], P(('sp', 'fsdp')), may hold values from 0.099609375 to 1.8984375
- frozen_key_weight: bfloat16 [4096, 512], P(('sp', 'fsdp')), may hold values from -0.09375 to 0.09375
- frozen_value_weight: bfloat16 [4096, 512], P(('sp', 'fsdp')), may hold values from -0.09375 to 0.09375
Outputs:
- policy_mixed: bfloat16 [4, 256, 1024], P(('groups', 'fsdp'), 'sp'), parts along dimension 0
- frozen_mixed: bfloat16 [4, 256, 1024], P(('groups', 'fsdp'), 'sp'), parts along dimension 0
The draws below stay inside these ranges and needn't reach their ends.
There are 2 independent parts, one for each index of `groups`. The reference program is written for one: setup_inputs(seed, part) draws one part's arguments, and reference() takes and returns one part's arrays. A program takes and returns all parts, laid end to end along the dimension named above; an argument that names none is the same for every part. Nothing has to cross between parts.
Inputs may be any that keep to these rules, and one draw needn't show every extreme that they name: `policy_documents`: along each sequence the ids never fall, and each document holds 1 to 128 positions. `frozen_documents`: along each sequence the ids never fall, and each document holds 1 to 128 positions.
All inputs are finite; a program needn't handle non-finite values.
Results may differ from the reference program's by a relative error of at most 0.007.
The reference program's roundings to bfloat16 on the way count: a program that leaves them out, or rounds other values in their place, can miss the bound.
Values may be sent and summed in bfloat16 or wider, within the bound.
A program may use at most 128 MiB of HBM per device.

```python
import math
import jax
import jax.numpy as jnp
import numpy as np
from jax import lax

D = 4096
HEAD_DIM = 128
KV_HEADS = 4
DOCS = 32
HEADS = 8
LENGTH = 256
DOC_MOST = 128
SEQS = 2


def query_draw(seed_key):
    standard = jax.random.normal(seed_key, (SEQS, LENGTH, HEADS, HEAD_DIM), jnp.float32)
    drawn = 2.5 * standard
    return jnp.clip(drawn, -512.0, 512.0).reshape(SEQS, LENGTH, HEADS * HEAD_DIM).astype(jnp.bfloat16)


def draw_policy_queries(key, part):
    return query_draw(jax.random.fold_in(key, 11))


def draw_frozen_queries(key, part):
    return query_draw(jax.random.fold_in(key, 23))


def levels(stream_key, dims, pieces, least, high):
    level, own = 1.0, jax.random.fold_in(stream_key, 6)
    for dim, blocks in pieces:
        steps = jnp.exp(jax.random.uniform(jax.random.fold_in(own, dim), (blocks,), jnp.float32, least / len(pieces), high / len(pieces)))
        level = level * jnp.repeat(steps, dims[dim] // blocks).reshape([-1 if axis == dim else 1 for axis in range(len(dims))])
    return level


def split_up(amount, total, limit, skew):
    portions = [(1 << 20) // math.isqrt(rank ** skew) + 1 for rank in range(2, amount + 1)]
    rest, counts = total - limit - (amount - 1), [1] * (amount - 1)
    while rest > 0:
        movable = [i for i in range(amount - 1) if counts[i] < limit]
        whole, budget = sum([portions[i] for i in movable]), rest
        for i in movable:
            extra = min(limit - counts[i], max(1, budget * portions[i] // whole), rest)
            counts[i] = counts[i] + extra
            rest = rest - extra
    return np.array([limit] + counts)


def ragged_sizes(own_key, count, total, bound, skew):
    if count == 2:
        one = jax.random.randint(own_key, (), max(1, total - bound), min(bound, total - 1) + 1)
        return jnp.stack([one, total - one])
    sizes = jnp.asarray(split_up(count, total, bound, skew), jnp.int32)
    pairs = (count - 1) // 2
    donor, sink = sizes[1:1 + 2 * pairs:2], sizes[2:2 + 2 * pairs:2]
    room = jnp.minimum(donor - 1, bound - sink)
    moved = jax.random.randint(jax.random.fold_in(own_key, 1), (pairs,), 0, 1 << 20) % (room + 1)
    sizes = sizes.at[1:1 + 2 * pairs:2].set(donor - moved).at[2:2 + 2 * pairs:2].set(sink + moved)
    return sizes[jax.random.permutation(jax.random.fold_in(own_key, 2), count)]


def bell_draw(key, shape, scale, reach, shards=(), kind=jnp.bfloat16):
    entries = scale * jax.random.normal(key, shape, jnp.float32)
    if shards:
        entries = entries * levels(key, shape, shards, -0.22, 0.18)
    return jnp.clip(entries, -reach, reach).astype(kind)


def setup_inputs(seed: int = 0, part: int = 0) -> dict:
    seeds = jax.random.split(jax.random.key(seed), 13)
    part_keys = jax.random.split(jax.random.fold_in(seeds[12], part), 13)
    policy_hidden = bell_draw(part_keys[0], (SEQS, LENGTH, D), 1.0, 6.0, ((0, 2), (1, 8)))
    policy_queries = draw_policy_queries(jax.random.fold_in(jax.random.fold_in(seeds[12], part), 71), part)
    policy_documents = jax.vmap(lambda own: jnp.searchsorted(jnp.cumsum(ragged_sizes(own, DOCS, LENGTH, DOC_MOST, 1)), jnp.arange(LENGTH), side="right"))(jax.random.split(part_keys[2], SEQS)).reshape((SEQS, LENGTH)).astype(jnp.int32)
    policy_gain = jnp.clip(1.0 + 0.18 * jax.random.normal(seeds[3], (D,), jnp.float32), 0.099609375, 1.8984375).astype(jnp.bfloat16)
    policy_key_weight = bell_draw(seeds[4], (D, KV_HEADS * HEAD_DIM), D ** -0.5, 0.09375, ((0, 16),))
    policy_value_weight = bell_draw(seeds[5], (D, KV_HEADS * HEAD_DIM), D ** -0.5, 0.09375, ((0, 16),))
    frozen_hidden = bell_draw(part_keys[6], (SEQS, LENGTH, D), 1.0, 6.0, ((0, 2), (1, 8)))
    frozen_queries = draw_frozen_queries(jax.random.fold_in(jax.random.fold_in(seeds[12], part), 71), part)
    frozen_documents = jax.vmap(lambda own: jnp.searchsorted(jnp.cumsum(ragged_sizes(own, DOCS, LENGTH, DOC_MOST, 1)), jnp.arange(LENGTH), side="right"))(jax.random.split(part_keys[8], SEQS)).reshape((SEQS, LENGTH)).astype(jnp.int32)
    frozen_gain = jnp.clip(1.0 + 0.18 * jax.random.normal(seeds[9], (D,), jnp.float32), 0.099609375, 1.8984375).astype(jnp.bfloat16)
    frozen_key_weight = bell_draw(seeds[10], (D, KV_HEADS * HEAD_DIM), D ** -0.5, 0.09375, ((0, 16),))
    frozen_value_weight = bell_draw(seeds[11], (D, KV_HEADS * HEAD_DIM), D ** -0.5, 0.09375, ((0, 16),))
    return {"policy_hidden": policy_hidden, "policy_queries": policy_queries, "policy_documents": policy_documents, "policy_gain": policy_gain, "policy_key_weight": policy_key_weight, "policy_value_weight": policy_value_weight, "frozen_hidden": frozen_hidden, "frozen_queries": frozen_queries, "frozen_documents": frozen_documents, "frozen_gain": frozen_gain, "frozen_key_weight": frozen_key_weight, "frozen_value_weight": frozen_value_weight}


EPS = 1e-05
ROPE_BASE = 500000.0
MASKED = -1e+30

def rotate(raw_keys, positions):
    half_dim = HEAD_DIM // 2
    frequency = jnp.exp(-jnp.log(ROPE_BASE) * jnp.arange(half_dim, dtype=jnp.float32) * 2.0 / HEAD_DIM)
    angles = positions.astype(jnp.float32)[:, None] * frequency[None, :]
    cosines = jnp.cos(angles)[:, None, :]
    sines = jnp.sin(angles)[:, None, :]
    front_half = raw_keys[..., :half_dim]
    back_half = raw_keys[..., half_dim:]
    return jnp.concatenate([front_half * cosines - back_half * sines, back_half * cosines + front_half * sines], axis=-1)

def one_model(hidden, queries, documents, gain, key_weight, value_weight):
    group_size = HEADS // KV_HEADS
    factor = HEAD_DIM ** (-0.5)
    block_rows = min(512, LENGTH)
    margin = min(512, LENGTH // 2)
    window = block_rows + margin

    def one_sequence(inputs):
        sequence, query_rows, doc_row = inputs
        widened = sequence.astype(jnp.float32)
        inverse = lax.rsqrt(lax.optimization_barrier(jnp.mean(widened * widened, axis=-1, keepdims=True)) + EPS)
        normed = (widened * inverse * gain.astype(jnp.float32)[None, :]).astype(jnp.bfloat16)
        positions = jnp.arange(LENGTH, dtype=jnp.int32)
        raw_keys = jnp.dot(normed, key_weight, preferred_element_type=jnp.float32).reshape(LENGTH, KV_HEADS, HEAD_DIM)
        key_heads = rotate(raw_keys, positions).astype(jnp.bfloat16)
        value_heads = jnp.dot(normed, value_weight, preferred_element_type=jnp.float32).astype(jnp.bfloat16).reshape(LENGTH, KV_HEADS, HEAD_DIM)
        query_heads = query_rows.reshape(LENGTH, HEADS, HEAD_DIM)
        padding = jnp.zeros((margin, KV_HEADS, HEAD_DIM), jnp.bfloat16)
        padded_keys = jnp.concatenate([padding, key_heads], axis=0)
        padded_values = jnp.concatenate([padding, value_heads], axis=0)
        padded_docs = jnp.concatenate([jnp.full((margin,), -1, jnp.int32), doc_row.astype(jnp.int32)], axis=0)
        offsets = jnp.arange(block_rows, dtype=jnp.int32)
        window_offsets = jnp.arange(window, dtype=jnp.int32)

        def one_block(block_index):
            first = (block_index * block_rows).astype(jnp.int32)
            query_block = lax.dynamic_slice_in_dim(query_heads, first, block_rows, 0).astype(jnp.float32)
            query_docs = lax.dynamic_slice_in_dim(doc_row.astype(jnp.int32), first, block_rows, 0)
            query_positions = first + offsets
            key_block = lax.dynamic_slice_in_dim(padded_keys, first, window, 0)
            value_block = lax.dynamic_slice_in_dim(padded_values, first, window, 0)
            key_docs = lax.dynamic_slice_in_dim(padded_docs, first, window, 0)
            key_positions = first - margin + window_offsets
            allowed = (key_positions[None, :] <= query_positions[:, None]) & (key_docs[None, :] == query_docs[:, None])
            wide_keys = jnp.repeat(key_block, group_size, axis=1).astype(jnp.float32)
            wide_values = jnp.repeat(value_block, group_size, axis=1).astype(jnp.float32)
            scores = jnp.einsum('qnd,knd->nqk', query_block, wide_keys) * factor
            scores = jnp.where(allowed[None], scores, MASKED)
            highest = lax.optimization_barrier(jnp.max(scores, axis=-1, keepdims=True))
            exponent = jnp.where(allowed[None], jnp.exp(scores - highest), 0.0)
            weights = (exponent / lax.optimization_barrier(jnp.sum(exponent, axis=-1, keepdims=True))).astype(jnp.bfloat16)
            return jnp.einsum('nqk,knd->qnd', weights.astype(jnp.float32), wide_values).astype(jnp.bfloat16)
        blocks = lax.map(one_block, jnp.arange(LENGTH // block_rows, dtype=jnp.int32))
        return blocks.reshape(LENGTH, HEADS * HEAD_DIM)
    return lax.map(one_sequence, (hidden, queries, documents))

def reference(policy_hidden, policy_queries, policy_documents, policy_gain, policy_key_weight, policy_value_weight, frozen_hidden, frozen_queries, frozen_documents, frozen_gain, frozen_key_weight, frozen_value_weight):
    policy_mixed = one_model(policy_hidden, policy_queries, policy_documents, policy_gain, policy_key_weight, policy_value_weight)
    frozen_mixed = one_model(frozen_hidden, frozen_queries, frozen_documents, frozen_gain, frozen_key_weight, frozen_value_weight)
    return (policy_mixed, frozen_mixed)
```

```python
import contextlib
import functools

import jax
import jax.numpy as jnp
import numpy as np
from jax import lax
from jax.experimental import pallas as pl
from jax.experimental.pallas import tpu as pltpu
from jax.sharding import PartitionSpec as P

HEAD_DIM = 128


EPS = 1e-05
ROPE_BASE = 500000.0
MASKED = -1e30


def rotate(raw_keys, positions):
    half_dim = HEAD_DIM // 2
    frequency = jnp.exp(
        -jnp.log(ROPE_BASE) * jnp.arange(half_dim, dtype=jnp.float32) * 2.0 / HEAD_DIM
    )
    angles = positions.astype(jnp.float32)[:, None] * frequency[None, :]
    cosines = jnp.cos(angles)[:, None, :]
    sines = jnp.sin(angles)[:, None, :]
    front_half = raw_keys[..., :half_dim]
    back_half = raw_keys[..., half_dim:]
    return jnp.concatenate(
        [front_half * cosines - back_half * sines, back_half * cosines + front_half * sines],
        axis=-1,
    )


def project(hidden, gain, key_weight, value_weight):
    tokens = hidden.shape[1]
    widened = hidden[0].astype(jnp.float32)
    inverse = lax.rsqrt(jnp.mean(widened * widened, axis=-1, keepdims=True) + EPS)
    scaled = widened * inverse
    gain_rows = lax.all_gather(gain, ("sp", "fsdp"), axis=0, tiled=True)
    key_rows = lax.all_gather(key_weight, ("sp", "fsdp"), axis=0, tiled=True)
    value_rows = lax.all_gather(value_weight, ("sp", "fsdp"), axis=0, tiled=True)
    normed = (scaled * gain_rows.astype(jnp.float32)[None, :]).astype(jnp.bfloat16)
    raw_keys = jnp.dot(normed, key_rows, preferred_element_type=jnp.float32)
    raw_values = jnp.dot(normed, value_rows, preferred_element_type=jnp.float32)
    positions = lax.axis_index("sp") * tokens + jnp.arange(tokens, dtype=jnp.int32)
    key_heads = rotate(raw_keys.reshape(tokens, -1, HEAD_DIM), positions).astype(jnp.bfloat16)
    value_heads = raw_values.astype(jnp.bfloat16).reshape(tokens, -1, HEAD_DIM)
    return (key_heads, value_heads)


def attend(queries, key_heads, value_heads, documents):
    length = queries.shape[0]
    head_count = queries.shape[1]
    block_rows = min(512, length)
    margin = min(512, length // 2)
    window = block_rows + margin
    factor = HEAD_DIM ** (-0.5)
    offsets = jnp.arange(block_rows, dtype=jnp.int32)
    window_offsets = jnp.arange(window, dtype=jnp.int32)
    padding = jnp.zeros((margin, head_count, HEAD_DIM), jnp.bfloat16)
    padded_keys = jnp.concatenate([padding, key_heads], axis=0)
    padded_values = jnp.concatenate([padding, value_heads], axis=0)
    padded_docs = jnp.concatenate([jnp.full((margin,), -1, jnp.int32), documents], axis=0)

    def one_block(block_index):
        first = block_index * block_rows
        query_block = lax.dynamic_slice_in_dim(queries, first, block_rows, 0)
        query_docs = lax.dynamic_slice_in_dim(documents, first, block_rows, 0)
        query_positions = first + offsets
        key_block = lax.dynamic_slice_in_dim(padded_keys, first, window, 0)
        value_block = lax.dynamic_slice_in_dim(padded_values, first, window, 0)
        key_docs = lax.dynamic_slice_in_dim(padded_docs, first, window, 0)
        key_positions = first - margin + window_offsets
        allowed = (key_positions[None, :] <= query_positions[:, None]) & (
            key_docs[None, :] == query_docs[:, None]
        )
        scores = (
            jnp.einsum("qnd,knd->nqk", query_block, key_block, preferred_element_type=jnp.float32)
            * factor
        )
        scores = jnp.where(allowed[None], scores, MASKED)
        highest = jnp.max(scores, axis=-1, keepdims=True)
        exponent = jnp.where(allowed[None], jnp.exp(scores - highest), 0.0)
        weights = (exponent / jnp.sum(exponent, axis=-1, keepdims=True)).astype(jnp.bfloat16)
        blended = jnp.einsum(
            "nqk,knd->qnd", weights, value_block, preferred_element_type=jnp.float32
        )
        return blended.astype(jnp.bfloat16)

    blocks = lax.map(one_block, jnp.arange(length // block_rows, dtype=jnp.int32))
    return blocks.reshape(length, head_count, HEAD_DIM)


def run_model(hidden, queries, documents, gain, key_weight, value_weight):
    tokens = hidden.shape[1]
    head_count = queries.shape[2] // HEAD_DIM
    query_local = queries[0].reshape(tokens, head_count, HEAD_DIM)
    every_doc = lax.all_gather(documents[0], "sp", axis=0, tiled=True)
    key_heads, value_heads = project(hidden, gain, key_weight, value_weight)
    group_size = head_count // key_heads.shape[1]
    wide_keys = jnp.repeat(key_heads, group_size, axis=1)
    wide_values = jnp.repeat(value_heads, group_size, axis=1)
    query_spread, key_spread, value_spread = (
        lax.all_to_all(query_local, "sp", split_axis=1, concat_axis=0, tiled=True),
        lax.all_to_all(wide_keys, "sp", split_axis=1, concat_axis=0, tiled=True),
        lax.all_to_all(wide_values, "sp", split_axis=1, concat_axis=0, tiled=True),
    )
    mixed = attend(query_spread, key_spread, value_spread, every_doc)
    returned = lax.all_to_all(mixed, "sp", split_axis=0, concat_axis=1, tiled=True)
    return returned.reshape(1, tokens, head_count * HEAD_DIM)


MESH = pl.DeviceIdType.MESH
TRACE = False


def fits(mesh, hidden, queries, key_weight):
    sp, cores = mesh.shape["sp"], mesh.shape["fsdp"]
    tokens = hidden.shape[1]
    kv_heads = key_weight.shape[1] // HEAD_DIM
    return (
        cores == 2
        and mesh.shape["groups"] == 2
        and sp == 8
        and kv_heads == 4
        and queries.shape[2] % (kv_heads * HEAD_DIM) == 0
        and key_weight.shape[0] % 128 == 0
        and hidden.shape[2] == key_weight.shape[0] * sp * cores
        and tokens % 16 == 0
        and tokens <= 64
    )


def fused_kernel(
    hidden0, hidden1, queries0, queries1, key0, key1, value0, value1, cosine_table, sine_table,
    gain0, gain1, documents0, documents1,
    out,
    gain_raw0, gain_raw1, doc_raw, near, rows, wide, normed, gain_send, gain_rows, row_send, row_data, query_rows, doc_wide,
    key_send, value_send, key_parts, value_parts, home, key_heads, value_heads, mixed, cosines, sines,
    raw_sem, near_sem, table_sem, send_sem, row_sem, wide_sem, gain_sem, data_sem, query_sem, part_sem, value_sem, out_sem,
):
    hiddens, queries = (hidden0, hidden1), (queries0, queries1)
    keys, values = (key0, key1), (value0, value1)
    tokens, features = hidden0.shape[1], key0.shape[0]
    slab = 8 * features
    head_cols = query_rows.shape[1]
    group_size = head_cols // HEAD_DIM
    length = query_rows.shape[0]
    sp, core, plane = lax.axis_index("sp"), lax.axis_index("fsdp"), lax.axis_index("groups")
    z, y = sp // 2, sp % 2
    upper, parity = z // 2, z % 2
    near_z = z + 1 - 2 * parity
    far_z = lax.rem(z + 2, 4)
    me = (plane * 8 + sp) * 2 + core

    barrier = pltpu.get_barrier_semaphore()
    for step in range(1, 32):
        other = lax.rem(me + step, 32)
        pl.semaphore_signal(
            barrier, inc=1, device_id={"groups": other // 16, "sp": (other // 2) % 8, "fsdp": other % 2},
            device_id_type=MESH,
        )

    def scope(name):
        return jax.named_scope(name) if TRACE else contextlib.nullcontext()

    def place(zz, yy, cc):
        return (zz * 2 + yy) * 2 + cc

    def place_rows(index):
        return pl.ds(pl.multiple_of(index * features, 128), features)

    mine = place(parity, y, core)

    def columns(half, b):
        return pl.ds(pl.multiple_of((half * 2 + b) * HEAD_DIM, HEAD_DIM), HEAD_DIM)

    for m in range(2):
        pltpu.make_async_copy(hiddens[m].at[0], near.at[m], near_sem.at[m]).start()

        @pl.when(plane == m)
        def _(m=m):
            for b in range(2):
                target = wide.at[b, place_rows(mine)]
                pltpu.make_async_copy(
                    keys[m].at[:, columns(y, b)], target.at[:, :HEAD_DIM], wide_sem.at[b, mine]
                ).start()
                pltpu.make_async_copy(
                    values[m].at[:, columns(y, b)], target.at[:, HEAD_DIM:], wide_sem.at[b, mine]
                ).start()

    small = (
        (gain0, gain_raw0), (gain1, gain_raw1), (documents0, doc_raw.at[0]), (documents1, doc_raw.at[1]),
    )
    for index, (src, dst) in enumerate(small):
        pltpu.make_async_copy(src, dst, raw_sem.at[index]).start()
    pltpu.make_async_copy(cosine_table, cosines, table_sem.at[0]).start()
    pltpu.make_async_copy(sine_table, sines, table_sem.at[1]).start()
    with scope("wbar"):
        pl.semaphore_wait(barrier, 31)

    pending = []

    def put(src, dst, recv, target, away=None):
        slot = len(pending)

        def make():
            return pltpu.make_async_remote_copy(
                src_ref=src, dst_ref=dst, send_sem=send_sem.at[slot], recv_sem=recv,
                device_id=target, device_id_type=MESH,
            )

        pending.append((away, make))
        if away is None:
            make().start()
        else:
            @pl.when(away)
            def _():
                make().start()

    def send(src, dst, recv, target, own):
        put(src, dst, recv, target, jnp.logical_not(own))

        @pl.when(own)
        def _():
            pltpu.make_async_copy(src, dst, recv).start()

    def put_weight(b, half, target):
        slot = len(pending)
        for index, weights in enumerate((keys, values)):
            cols = slice(index * HEAD_DIM, (index + 1) * HEAD_DIM)

            def make(m, index=index, weights=weights, cols=cols):
                return pltpu.make_async_remote_copy(
                    src_ref=weights[m].at[:, columns(half, b)], dst_ref=wide.at[b, place_rows(mine), cols],
                    send_sem=send_sem.at[slot + index], recv_sem=wide_sem.at[b, mine],
                    device_id=target, device_id_type=MESH,
                )

            for m in range(2):
                @pl.when(plane == m)
                def _(m=m, make=make):
                    make(m).start()
            pending.append((None, functools.partial(make, 0)))

    def arrive(dst, recv, name):
        with scope(name):
            pltpu.make_async_copy(dst, dst, recv).wait()

    def forward(b, index, targets):
        block = wide.at[b, place_rows(index)]
        for target in targets:
            put(block, block, wide_sem.at[b, index], target)

    def arrive_weight(b, index, name):
        block = wide.at[b, place_rows(index)]
        arrive(block, wide_sem.at[b, index], name)

    across, beside, along = {"sp": z * 2 + 1 - y}, {"fsdp": 1 - core}, {"sp": near_z * 2 + y}
    beyond = {"sp": near_z * 2 + 1 - y}
    away_head, home_head = 1 - upper, upper

    put_weight(away_head, 1 - y, across)
    put_weight(away_head, y, along)
    put_weight(away_head, 1 - y, beyond)
    put_weight(away_head, y, beside)
    put_weight(home_head, 1 - y, across)
    for m in range(2):
        pltpu.make_async_copy(hiddens[m].at[0], near.at[m], near_sem.at[m]).wait()

    def put_hidden(h):
        to_z = 2 * h + core
        for other in range(2):
            m = plane if other == 0 else 1 - plane
            src, dst = near.at[m, :, pl.ds(pl.multiple_of(h * slab, 128), slab)], rows.at[sp]
            target = {"groups": m, "sp": to_z * 2 + y, "fsdp": plane}
            if other:
                put(src, dst, row_sem.at[sp], target)
            else:
                send(src, dst, row_sem.at[sp], target, (to_z == z) & (core == plane))

    for index, (src, dst) in enumerate(small):
        pltpu.make_async_copy(src, dst, raw_sem.at[index]).wait()
    gain_send[...] = jnp.where(
        plane == 0, gain_raw0[...].astype(jnp.float32), gain_raw1[...].astype(jnp.float32)
    ).reshape(1, -1)
    for zz in range(2):
        for yy in range(2):
            for cc in range(2):
                own = (parity == zz) & (y == yy) & (core == cc)
                send(
                    gain_send, gain_rows.at[mine], gain_sem,
                    {"sp": (upper * 2 + zz) * 2 + yy, "fsdp": cc}, own,
                )
    square = (
        lax.broadcasted_iota(jnp.int32, (tokens, 128), 0)
        == lax.broadcasted_iota(jnp.int32, (tokens, 128), 1)
    )
    for m in range(2):
        wide_row = near[m].astype(jnp.float32)
        inverse = lax.rsqrt(jnp.mean(wide_row * wide_row, axis=-1, keepdims=True) + EPS)
        row_send[m] = jnp.zeros((8, 128), jnp.float32)
        row_send[m, 0:1, :] = jnp.sum(jnp.where(square, inverse, 0.0), axis=0, keepdims=True)
        row_send[m, 1:2, :tokens] = doc_raw[m].astype(jnp.float32)
    for m in range(2):
        for yy in range(2):
            for h in range(2):
                to_z = 2 * h + core
                send(
                    row_send.at[m], row_data.at[sp], data_sem,
                    {"groups": m, "sp": to_z * 2 + yy, "fsdp": plane},
                    (plane == m) & (y == yy) & (to_z == z) & (core == plane),
                )
    put_hidden(upper)
    put_hidden(1 - upper)
    put_weight(home_head, y, along)
    put_weight(home_head, y, beside)

    place_y, place_z, place_zy = place(parity, 1 - y, core), place(1 - parity, y, core), place(1 - parity, 1 - y, core)

    def pass_rows(step):
        from_z = order[step]
        block = from_z * 2 + y
        arrive(rows.at[block], row_sem.at[block], f"whid{step}")
        put(rows.at[block], rows.at[block], row_sem.at[block], across)

    order = (z, near_z + upper * (1 - near_z), 2 * (1 - upper), 3 + upper * (near_z - 3))
    pass_rows(0)
    arrive_weight(away_head, place_y, "wy0")
    forward(away_head, place_y, (beside,))
    arrive_weight(away_head, place_z, "wz0")
    forward(away_head, place_z, (beside,))
    arrive_weight(away_head, place_zy, "wzy0")
    forward(away_head, place_zy, (beside,))
    arrive_weight(home_head, place_y, "wy1")
    forward(home_head, place_y, (along, beside))
    pass_rows(1)
    arrive(gain_rows, gain_sem, "wgain")
    arrive(row_data, data_sem, "wdata")
    arrive_weight(away_head, mine, "wown0")
    for zz in range(2):
        for yy in range(2):
            arrive_weight(away_head, place(zz, yy, 1 - core), "wside0")
    gain_row = jnp.concatenate([gain_rows[s] for s in range(8)], axis=1)
    partner = {"sp": far_z * 2 + y}

    def block_of(index, k):
        return index // 2 * 4 + 2 * k + (y if index % 2 == 0 else 1 - y)

    def project(index):
        for k in range(2):
            s = block_of(index, k)
            scale = jnp.sum(jnp.where(square, row_data[s, 0:1, :], 0.0), axis=1, keepdims=True)
            normed[index, k * tokens:(k + 1) * tokens, :] = (
                rows[s].astype(jnp.float32) * scale * gain_row
            ).astype(jnp.bfloat16)
        part = jnp.dot(normed[index], wide[away_head], preferred_element_type=jnp.float32)
        key_send[index] = part[:, :HEAD_DIM]
        value_send[index] = part[:, HEAD_DIM:].astype(jnp.bfloat16)
        put(key_send.at[index], key_parts.at[index], part_sem.at[index], partner)
        put(value_send.at[index], value_parts.at[index], value_sem.at[index], partner)

    def arrive_rows(index):
        for k in range(2):
            block = block_of(index, k)
            arrive(rows.at[block], row_sem.at[block], f"wfwd{index}")

    pass_rows(2)
    project(0)
    pass_rows(3)
    arrive_rows(1)
    project(1)
    token_rows = pl.ds(pl.multiple_of(sp * tokens, 16), tokens)
    for m in range(2):
        for yy in range(2):
            for h in range(2):
                to_z, head = 2 * h + core, yy * 2 + h
                send(
                    queries[m].at[0, :, head * head_cols:(head + 1) * head_cols],
                    query_rows.at[token_rows], query_sem.at[upper],
                    {"groups": m, "sp": to_z * 2 + yy, "fsdp": plane},
                    (plane == m) & (y == yy) & (to_z == z) & (core == plane),
                )

    project(2)
    arrive_weight(home_head, place_z, "wz1")
    forward(home_head, place_z, (beside,))
    arrive_rows(3)
    project(3)

    for s in range(8):
        column = jnp.sum(jnp.where(square, row_data[s, 1:2, :], 0.0), axis=1, keepdims=True)
        doc_wide[s * tokens:(s + 1) * tokens, :] = jnp.broadcast_to(column, (tokens, 128))
    query_index = lax.broadcasted_iota(jnp.int32, (length, length), 0)
    key_index = lax.broadcasted_iota(jnp.int32, (length, length), 1)
    doc_column = doc_wide[:, :1]
    doc_row = jnp.sum(jnp.where(query_index == key_index, doc_column, 0.0), axis=0, keepdims=True)
    arrive_weight(home_head, place_zy, "wzy1")
    forward(home_head, place_zy, (beside,))
    for index in range(2):
        pltpu.make_async_copy((cosine_table, sine_table)[index], (cosines, sines)[index], table_sem.at[index]).wait()
    arrive_weight(home_head, mine, "wown1")
    for zz in range(2):
        for yy in range(2):
            arrive_weight(home_head, place(zz, yy, 1 - core), "wside1")

    for index in range(4):
        own_part = jnp.dot(normed[index], wide[home_head], preferred_element_type=jnp.float32)
        for k in range(2):
            block = pl.ds(pl.multiple_of(block_of(index, k) * tokens, 16), tokens)
            home[block, :] = own_part[k * tokens:(k + 1) * tokens, :]
    factor = HEAD_DIM ** (-0.5)
    head = y * 2 + upper
    out_columns = pl.ds(pl.multiple_of(head * head_cols, 128), head_cols)
    half_rows = length // 2
    for half in range(2):
        for index in range(2 * half, 2 * half + 2):
            arrive(key_parts.at[index], part_sem.at[index], f"wpart{index}")
            arrive(value_parts.at[index], value_sem.at[index], f"wpart{index}")
            for k in range(2):
                block = pl.ds(pl.multiple_of(block_of(index, k) * tokens, 16), tokens)
                near_rows = slice(k * tokens, (k + 1) * tokens)
                raw_keys = home[block, :HEAD_DIM] + key_parts[index, near_rows, :]
                raw_values = home[block, HEAD_DIM:] + value_parts[index, near_rows, :].astype(jnp.float32)
                key_heads[block, :] = (
                    raw_keys * cosines[block, :] + pltpu.roll(raw_keys, HEAD_DIM // 2, 1) * sines[block, :]
                ).astype(jnp.bfloat16)
                value_heads[block, :] = raw_values.astype(jnp.bfloat16)
        first, last = half * half_rows, (half + 1) * half_rows
        arrive(query_rows.at[first:last], query_sem.at[half], f"wq{half}")
        allowed = (
            lax.broadcasted_iota(jnp.int32, (half_rows, last), 1)
            <= first + lax.broadcasted_iota(jnp.int32, (half_rows, last), 0)
        ) & (doc_row[:, :last] == doc_wide[first:last, :1])
        for g in range(group_size):
            cols = slice(g * HEAD_DIM, (g + 1) * HEAD_DIM)
            scores = lax.dot_general(
                query_rows[first:last, cols], key_heads[:last, :], (((1,), (1,)), ((), ())),
                preferred_element_type=jnp.float32,
            ) * factor
            scores = jnp.where(allowed, scores, MASKED)
            highest = jnp.max(scores, axis=-1, keepdims=True)
            exponent = jnp.where(allowed, jnp.exp(scores - highest), 0.0)
            weights = (exponent / jnp.sum(exponent, axis=-1, keepdims=True)).astype(jnp.bfloat16)
            mixed[half, :, cols] = jnp.dot(
                weights, value_heads[:last, :], preferred_element_type=jnp.float32
            ).astype(jnp.bfloat16)
        for k in range(4):
            to_sp = half * 4 + k
            send(
                mixed.at[half, k * tokens:(k + 1) * tokens], out.at[plane, 0, :, out_columns], out_sem,
                {"groups": core, "sp": to_sp, "fsdp": parity},
                (core == plane) & (sp == to_sp) & (core == parity),
            )
    with scope("wsend"):
        for away, make in pending:
            if away is None:
                make().wait_send()
            else:
                @pl.when(away)
                def _(make=make):
                    make().wait_send()
    arrive(out, out_sem, "wout")


def fused(mesh, hiddens, queries, documents, gains, keys, values):
    sp = mesh.shape["sp"]
    tokens, features = hiddens[0].shape[1], keys[0].shape[0]
    kv_heads = keys[0].shape[1] // HEAD_DIM
    head_cols = queries[0].shape[2] // kv_heads
    length = sp * tokens
    half_dim = HEAD_DIM // 2
    frequency = ROPE_BASE ** (-2.0 * np.arange(half_dim) / HEAD_DIM)
    angles = np.arange(length)[:, None] * frequency[None, :]
    cosines = np.concatenate([np.cos(angles), np.cos(angles)], axis=1).astype(np.float32)
    sines = np.concatenate([-np.sin(angles), np.sin(angles)], axis=1).astype(np.float32)
    dma = pltpu.SemaphoreType.DMA
    bf16, f32 = jnp.bfloat16, jnp.float32
    sends = 14 + 4 + 8 + 8 + 8 + 4 + 8 + 8 + 8
    out = pl.pallas_call(
        fused_kernel,
        out_shape=pltpu.VMEM((2, 1, tokens, queries[0].shape[2]), bf16),
        in_specs=[pl.BlockSpec(memory_space=pl.ANY)] * 14,
        out_specs=pl.BlockSpec(memory_space=pltpu.VMEM),
        scratch_shapes=[
            pltpu.VMEM((features,), bf16),
            pltpu.VMEM((features,), bf16),
            pltpu.VMEM((2, 1, tokens), jnp.int32),
            pltpu.VMEM((2,) + hiddens[0].shape[1:], bf16),
            pltpu.VMEM((sp, tokens, 8 * features), bf16),
            pltpu.VMEM((2, 8 * features, 2 * HEAD_DIM), bf16),
            pltpu.VMEM((4, 2 * tokens, 8 * features), bf16),
            pltpu.VMEM((1, features), f32),
            pltpu.VMEM((8, 1, features), f32),
            pltpu.VMEM((2, 8, 128), f32),
            pltpu.VMEM((sp, 8, 128), f32),
            pltpu.VMEM((length, head_cols), bf16),
            pltpu.VMEM((length, 128), f32),
            pltpu.VMEM((4, 2 * tokens, HEAD_DIM), f32),
            pltpu.VMEM((4, 2 * tokens, HEAD_DIM), bf16),
            pltpu.VMEM((4, 2 * tokens, HEAD_DIM), f32),
            pltpu.VMEM((4, 2 * tokens, HEAD_DIM), bf16),
            pltpu.VMEM((length, 2 * HEAD_DIM), f32),
            pltpu.VMEM((length, HEAD_DIM), bf16),
            pltpu.VMEM((length, HEAD_DIM), bf16),
            pltpu.VMEM((2, length // 2, head_cols), bf16),
            pltpu.VMEM((length, HEAD_DIM), f32),
            pltpu.VMEM((length, HEAD_DIM), f32),
            dma((4,)),
            dma((2,)),
            dma((2,)),
            dma((sends,)),
            dma((sp,)),
            dma((2, 8)),
            dma(()),
            dma(()),
            dma((2,)),
            dma((4,)),
            dma((4,)),
            dma(()),
        ],
        compiler_params=pltpu.CompilerParams(collective_id=0, has_side_effects=True),
        name="fused",
    )(
        *hiddens, *queries, *keys, *values, cosines, sines,
        *gains, *documents,
    )
    return out[0], out[1]


def per_device(
    mesh,
    policy_hidden,
    policy_queries,
    policy_documents,
    policy_gain,
    policy_key_weight,
    policy_value_weight,
    frozen_hidden,
    frozen_queries,
    frozen_documents,
    frozen_gain,
    frozen_key_weight,
    frozen_value_weight,
):
    if fits(mesh, policy_hidden, policy_queries, policy_key_weight):
        return fused(
            mesh,
            (policy_hidden, frozen_hidden),
            (policy_queries, frozen_queries),
            (policy_documents, frozen_documents),
            (policy_gain, frozen_gain),
            (policy_key_weight, frozen_key_weight),
            (policy_value_weight, frozen_value_weight),
        )
    policy_mixed = run_model(
        policy_hidden,
        policy_queries,
        policy_documents,
        policy_gain,
        policy_key_weight,
        policy_value_weight,
    )
    frozen_mixed = run_model(
        frozen_hidden,
        frozen_queries,
        frozen_documents,
        frozen_gain,
        frozen_key_weight,
        frozen_value_weight,
    )
    return (policy_mixed, frozen_mixed)


def solution(mesh):
    return jax.shard_map(
        functools.partial(per_device, mesh),
        mesh=mesh,
        in_specs=(
            P(("groups", "fsdp"), "sp", None),
            P(("groups", "fsdp"), "sp", None),
            P(("groups", "fsdp"), "sp"),
            P(("sp", "fsdp")),
            P(("sp", "fsdp"), None),
            P(("sp", "fsdp"), None),
            P(("groups", "fsdp"), "sp", None),
            P(("groups", "fsdp"), "sp", None),
            P(("groups", "fsdp"), "sp"),
            P(("sp", "fsdp")),
            P(("sp", "fsdp"), None),
            P(("sp", "fsdp"), None),
        ),
        out_specs=(P(("groups", "fsdp"), "sp", None), P(("groups", "fsdp"), "sp", None)),
        check_vma=False,
    )
```

```python
import contextlib
import functools

import jax
import jax.numpy as jnp
import numpy as np
from jax import lax
from jax.experimental import pallas as pl
from jax.experimental.pallas import tpu as pltpu
from jax.sharding import PartitionSpec as P

HEAD_DIM = 128


EPS = 1e-05
ROPE_BASE = 500000.0
MASKED = -1e30


def rotate(raw_keys, positions):
    half_dim = HEAD_DIM // 2
    frequency = jnp.exp(
        -jnp.log(ROPE_BASE) * jnp.arange(half_dim, dtype=jnp.float32) * 2.0 / HEAD_DIM
    )
    angles = positions.astype(jnp.float32)[:, None] * frequency[None, :]
    cosines = jnp.cos(angles)[:, None, :]
    sines = jnp.sin(angles)[:, None, :]
    front_half = raw_keys[..., :half_dim]
    back_half = raw_keys[..., half_dim:]
    return jnp.concatenate(
        [front_half * cosines - back_half * sines, back_half * cosines + front_half * sines],
        axis=-1,
    )


def project(hidden, gain, key_weight, value_weight):
    tokens = hidden.shape[1]
    widened = hidden[0].astype(jnp.float32)
    inverse = lax.rsqrt(jnp.mean(widened * widened, axis=-1, keepdims=True) + EPS)
    scaled = widened * inverse
    gain_rows = lax.all_gather(gain, ("sp", "fsdp"), axis=0, tiled=True)
    key_rows = lax.all_gather(key_weight, ("sp", "fsdp"), axis=0, tiled=True)
    value_rows = lax.all_gather(value_weight, ("sp", "fsdp"), axis=0, tiled=True)
    normed = (scaled * gain_rows.astype(jnp.float32)[None, :]).astype(jnp.bfloat16)
    raw_keys = jnp.dot(normed, key_rows, preferred_element_type=jnp.float32)
    raw_values = jnp.dot(normed, value_rows, preferred_element_type=jnp.float32)
    positions = lax.axis_index("sp") * tokens + jnp.arange(tokens, dtype=jnp.int32)
    key_heads = rotate(raw_keys.reshape(tokens, -1, HEAD_DIM), positions).astype(jnp.bfloat16)
    value_heads = raw_values.astype(jnp.bfloat16).reshape(tokens, -1, HEAD_DIM)
    return (key_heads, value_heads)


def attend(queries, key_heads, value_heads, documents):
    length = queries.shape[0]
    head_count = queries.shape[1]
    block_rows = min(512, length)
    margin = min(512, length // 2)
    window = block_rows + margin
    factor = HEAD_DIM ** (-0.5)
    offsets = jnp.arange(block_rows, dtype=jnp.int32)
    window_offsets = jnp.arange(window, dtype=jnp.int32)
    padding = jnp.zeros((margin, head_count, HEAD_DIM), jnp.bfloat16)
    padded_keys = jnp.concatenate([padding, key_heads], axis=0)
    padded_values = jnp.concatenate([padding, value_heads], axis=0)
    padded_docs = jnp.concatenate([jnp.full((margin,), -1, jnp.int32), documents], axis=0)

    def one_block(block_index):
        first = block_index * block_rows
        query_block = lax.dynamic_slice_in_dim(queries, first, block_rows, 0)
        query_docs = lax.dynamic_slice_in_dim(documents, first, block_rows, 0)
        query_positions = first + offsets
        key_block = lax.dynamic_slice_in_dim(padded_keys, first, window, 0)
        value_block = lax.dynamic_slice_in_dim(padded_values, first, window, 0)
        key_docs = lax.dynamic_slice_in_dim(padded_docs, first, window, 0)
        key_positions = first - margin + window_offsets
        allowed = (key_positions[None, :] <= query_positions[:, None]) & (
            key_docs[None, :] == query_docs[:, None]
        )
        scores = (
            jnp.einsum("qnd,knd->nqk", query_block, key_block, preferred_element_type=jnp.float32)
            * factor
        )
        scores = jnp.where(allowed[None], scores, MASKED)
        highest = jnp.max(scores, axis=-1, keepdims=True)
        exponent = jnp.where(allowed[None], jnp.exp(scores - highest), 0.0)
        weights = (exponent / jnp.sum(exponent, axis=-1, keepdims=True)).astype(jnp.bfloat16)
        blended = jnp.einsum(
            "nqk,knd->qnd", weights, value_block, preferred_element_type=jnp.float32
        )
        return blended.astype(jnp.bfloat16)

    blocks = lax.map(one_block, jnp.arange(length // block_rows, dtype=jnp.int32))
    return blocks.reshape(length, head_count, HEAD_DIM)


def run_model(hidden, queries, documents, gain, key_weight, value_weight):
    tokens = hidden.shape[1]
    head_count = queries.shape[2] // HEAD_DIM
    query_local = queries[0].reshape(tokens, head_count, HEAD_DIM)
    every_doc = lax.all_gather(documents[0], "sp", axis=0, tiled=True)
    key_heads, value_heads = project(hidden, gain, key_weight, value_weight)
    group_size = head_count // key_heads.shape[1]
    wide_keys = jnp.repeat(key_heads, group_size, axis=1)
    wide_values = jnp.repeat(value_heads, group_size, axis=1)
    query_spread, key_spread, value_spread = (
        lax.all_to_all(query_local, "sp", split_axis=1, concat_axis=0, tiled=True),
        lax.all_to_all(wide_keys, "sp", split_axis=1, concat_axis=0, tiled=True),
        lax.all_to_all(wide_values, "sp", split_axis=1, concat_axis=0, tiled=True),
    )
    mixed = attend(query_spread, key_spread, value_spread, every_doc)
    returned = lax.all_to_all(mixed, "sp", split_axis=0, concat_axis=1, tiled=True)
    return returned.reshape(1, tokens, head_count * HEAD_DIM)


MESH = pl.DeviceIdType.MESH
TRACE = False


def fits(mesh, hidden, queries, key_weight):
    sp, cores = mesh.shape["sp"], mesh.shape["fsdp"]
    tokens = hidden.shape[1]
    kv_heads = key_weight.shape[1] // HEAD_DIM
    return (
        cores == 2
        and mesh.shape["groups"] == 2
        and sp == 8
        and kv_heads == 4
        and queries.shape[2] % (kv_heads * HEAD_DIM) == 0
        and key_weight.shape[0] % 128 == 0
        and hidden.shape[2] == key_weight.shape[0] * sp * cores
        and tokens % 16 == 0
        and tokens <= 64
    )


def fused_kernel(
    hidden0, hidden1, queries0, queries1, key0, key1, value0, value1, table,
    gain0, gain1, documents0, documents1,
    out,
    gain_raw0, gain_raw1, doc_raw, near, rows, wide, normed, gain_send, gain_rows, row_send, row_data, query_rows, doc_wide,
    key_send, value_send, key_parts, value_parts, home, key_heads, value_heads, mixed, tables,
    ready, raw_sem, near_sem, table_sem, send_sem, row_sem, wide_sem, side_sem, gain_sem, data_sem, query_sem, part_sem, value_sem, out_sem,
):
    hiddens, queries = (hidden0, hidden1), (queries0, queries1)
    keys, values = (key0, key1), (value0, value1)
    tokens, features = hidden0.shape[1], key0.shape[0]
    slab = 8 * features
    head_cols = query_rows.shape[1]
    group_size = head_cols // HEAD_DIM
    length = query_rows.shape[0]
    sp, core, plane = lax.axis_index("sp"), lax.axis_index("fsdp"), lax.axis_index("groups")
    z, y = sp // 2, sp % 2
    upper, parity = z // 2, z % 2
    near_z = z + 1 - 2 * parity
    far_z = lax.rem(z + 2, 4)

    def scope(name):
        return jax.named_scope(name) if TRACE else contextlib.nullcontext()

    inner = upper != parity
    greeted = 6 + 2 * jnp.where(inner, 1, 0)

    def greet(semaphore):
        for c in range(2):
            pl.semaphore_signal(
                semaphore, inc=1, device_id={"groups": 1 - plane, "fsdp": c}, device_id_type=MESH
            )
            pl.semaphore_signal(
                semaphore, inc=1, device_id={"sp": near_z * 2 + y, "fsdp": c}, device_id_type=MESH
            )

            @pl.when(inner)
            def _(c=c):
                pl.semaphore_signal(
                    semaphore, inc=1, device_id={"sp": (3 - z) * 2 + y, "fsdp": c}, device_id_type=MESH
                )
        pl.semaphore_signal(semaphore, inc=1, device_id={"sp": z * 2 + 1 - y}, device_id_type=MESH)
        pl.semaphore_signal(semaphore, inc=1, device_id={"fsdp": 1 - core}, device_id_type=MESH)

    barrier = pltpu.get_barrier_semaphore()
    greet(barrier)

    def place(zz, yy, cc):
        return (zz * 2 + yy) * 2 + cc

    def place_rows(index):
        return pl.ds(pl.multiple_of(index * features, 128), features)

    mine = place(parity, y, core)
    own_any = (core == plane) & (core == parity)

    def columns(half, b):
        return pl.ds(pl.multiple_of((half * 2 + b) * HEAD_DIM, HEAD_DIM), HEAD_DIM)

    for m in range(2):
        pltpu.make_async_copy(hiddens[m].at[0], near.at[m], near_sem).start()
    small = (
        (gain0, gain_raw0), (gain1, gain_raw1), (documents0, doc_raw.at[0]), (documents1, doc_raw.at[1]),
    )
    for index, (src, dst) in enumerate(small):
        pltpu.make_async_copy(src, dst, raw_sem.at[index]).start()
    with scope("wbar"):
        pl.semaphore_wait(barrier, greeted)
    greet(ready.at[0])

    def next_round(step):
        with scope(f"wround{step}"):
            pl.semaphore_wait(ready.at[step], greeted)
        if step < 3:
            greet(ready.at[step + 1])

    def put(src, dst, recv, target, sent, away=None):
        def start():
            pltpu.make_async_remote_copy(
                src_ref=src, dst_ref=dst, send_sem=send_sem.at[sent], recv_sem=recv,
                device_id=target, device_id_type=MESH,
            ).start()

        if away is None:
            start()
        else:
            pl.when(away)(start)

    def send(src, dst, recv, target, sent, own):
        put(src, dst, recv, target, sent, jnp.logical_not(own))

        @pl.when(own)
        def _():
            pltpu.make_async_copy(src, dst, recv).start()

    def put_weight(b, half, target, sent, recv):
        for index, weights in enumerate((keys, values)):
            cols = slice(index * HEAD_DIM, (index + 1) * HEAD_DIM)
            for m in range(2):
                put(
                    weights[m].at[:, columns(half, b)], wide.at[b, place_rows(mine), cols], recv,
                    target, sent, plane == m,
                )

    def arrive(dst, recv, name):
        with scope(name):
            pltpu.make_async_copy(dst, dst, recv).wait()

    def lane(zz, yy):
        return zz * 2 + yy

    def forward(b, zz, yy, sent, further=None):
        block = wide.at[b, place_rows(place(zz, yy, core))]
        arrive(block, wide_sem.at[b, lane(zz, yy)], "wweight")
        put(block, block, side_sem.at[b], beside, sent)
        if further is not None:
            put(block, block, wide_sem.at[b, lane(zz, yy)], further, sent)

    def arrive_own(b):
        arrive(wide.at[b, place_rows(mine)], wide_sem.at[b, lane(parity, y)], "wown")

    def arrive_side(b):
        arrive(wide.at[b, :4 * features], side_sem.at[b], "wside")

    across, beside, along = {"sp": z * 2 + 1 - y}, {"fsdp": 1 - core}, {"sp": near_z * 2 + y}
    beyond = {"sp": near_z * 2 + 1 - y}
    away_head, home_head = 1 - upper, upper

    own_lane = lane(parity, y)
    put_weight(away_head, 1 - y, across, 0, wide_sem.at[away_head, own_lane])
    put_weight(away_head, y, along, 0, wide_sem.at[away_head, own_lane])
    put_weight(away_head, y, beside, 0, side_sem.at[away_head])
    put_weight(home_head, 1 - y, across, 0, wide_sem.at[home_head, own_lane])
    for m in range(2):
        @pl.when(plane == m)
        def _(m=m):
            for b in range(2):
                target = wide.at[b, place_rows(mine)]
                pltpu.make_async_copy(
                    keys[m].at[:, columns(y, b)], target.at[:, :HEAD_DIM], wide_sem.at[b, parity * 2 + y]
                ).start()
                pltpu.make_async_copy(
                    values[m].at[:, columns(y, b)], target.at[:, HEAD_DIM:], wide_sem.at[b, parity * 2 + y]
                ).start()

    pltpu.make_async_copy(table, tables, table_sem).start()
    pltpu.make_async_copy(near, near, near_sem).wait()

    def put_hidden(h, other, when=None):
        to_z = 2 * h + core
        m = 1 - plane if other else plane
        src, dst = near.at[m, :, pl.ds(pl.multiple_of(h * slab, 128), slab)], rows.at[sp]
        target = {"groups": m, "sp": to_z * 2 + y, "fsdp": plane}
        if other:
            put(src, dst, row_sem.at[sp], target, 2, when)
        else:
            own = (to_z == z) & (core == plane)
            send(src, dst, row_sem.at[sp], target, 2, own)

    for index, (src, dst) in enumerate(small):
        pltpu.make_async_copy(src, dst, raw_sem.at[index]).wait()
    put_hidden(upper, True, core == parity)
    square = (
        lax.broadcasted_iota(jnp.int32, (tokens, 128), 0)
        == lax.broadcasted_iota(jnp.int32, (tokens, 128), 1)
    )
    for m in range(2):
        wide_row = near[m].astype(jnp.float32)
        inverse = lax.rsqrt(jnp.mean(wide_row * wide_row, axis=-1, keepdims=True) + EPS)
        row_send[m] = jnp.sum(jnp.where(square, inverse, 0.0), axis=0, keepdims=True)
        row_send[m, :, 64:64 + tokens] = doc_raw[m].astype(jnp.float32)
    next_round(0)
    put_weight(away_head, 1 - y, beyond, 0, wide_sem.at[away_head, own_lane])
    gain_send[...] = jnp.where(
        plane == 0, gain_raw0[...].astype(jnp.float32), gain_raw1[...].astype(jnp.float32)
    ).reshape(1, -1)
    for zz in range(2):
        for yy in range(2):
            for cc in range(2):
                own = (parity == zz) & (y == yy) & (core == cc)
                send(
                    gain_send, gain_rows.at[mine], gain_sem,
                    {"sp": (upper * 2 + zz) * 2 + yy, "fsdp": cc}, 3, own,
                )
    put_hidden(upper, False)

    def put_queries():
        token_rows = pl.ds(pl.multiple_of(sp * tokens, 16), tokens)
        for m in range(2):
            for yy in range(2):
                for h in range(2):
                    to_z, head = 2 * h + core, yy * 2 + h
                    send(
                        queries[m].at[0, :, head * head_cols:(head + 1) * head_cols],
                        query_rows.at[token_rows], query_sem.at[upper],
                        {"groups": m, "sp": to_z * 2 + yy, "fsdp": plane}, 5,
                        (plane == m) & (y == yy) & (to_z == z) & (core == plane),
                    )

    def put_row_data(h):
        to_z = 2 * h + core
        for m in range(2):
            for yy in range(2):
                send(
                    row_send.at[m], row_data.at[sp], data_sem.at[upper],
                    {"groups": m, "sp": to_z * 2 + yy, "fsdp": plane}, 4,
                    (plane == m) & (y == yy) & (to_z == z) & (core == plane),
                )

    next_round(1)
    put_row_data(upper)
    put_hidden(upper, True, core != parity)
    put_hidden(1 - upper, False)
    next_round(2)
    next_round(3)
    put_row_data(1 - upper)
    put_hidden(1 - upper, True)
    put_queries()
    put_weight(home_head, y, along, 1, wide_sem.at[home_head, own_lane])
    put_weight(home_head, y, beside, 1, side_sem.at[home_head])


    def pass_rows(step):
        from_z = order[step]
        block = from_z * 2 + y
        arrive(rows.at[block], row_sem.at[block], f"whid{step}")
        put(rows.at[block], rows.at[block], row_sem.at[block], across, 6)

    order = (z, near_z + upper * (1 - near_z), 2 * (1 - upper), 3 + upper * (near_z - 3))
    pass_rows(0)
    forward(away_head, parity, 1 - y, 0)
    forward(away_head, 1 - parity, y, 0)
    forward(away_head, 1 - parity, 1 - y, 0)
    forward(home_head, parity, 1 - y, 1, along)
    pass_rows(1)
    pass_rows(2)
    arrive(gain_rows, gain_sem, "wgain")
    arrive_own(away_head)
    arrive_side(away_head)
    gain_row = jnp.concatenate([gain_rows[s] for s in range(8)], axis=1)
    partner = {"sp": far_z * 2 + y}

    def block_of(index, k):
        return index // 2 * 4 + 2 * k + (y if index % 2 == 0 else 1 - y)

    def project(index):
        if index % 2 == 0:
            arrive(row_data.at[2 * index:2 * index + 4], data_sem.at[index // 2], f"wdata{index}")
        for k in range(2):
            s = block_of(index, k)
            scale = jnp.sum(jnp.where(square, row_data[s], 0.0), axis=1, keepdims=True)
            spot = (index % 2 * 2 + k) * tokens
            normed[index // 2, spot:spot + tokens, :] = (
                rows[s].astype(jnp.float32) * scale * gain_row
            ).astype(jnp.bfloat16)
        spot = index % 2 * 2 * tokens
        part = jnp.dot(
            normed[index // 2, spot:spot + 2 * tokens, :], wide[away_head], preferred_element_type=jnp.float32
        )
        key_send[index] = part[:, :HEAD_DIM]
        value_send[index] = part[:, HEAD_DIM:].astype(jnp.bfloat16)
        put(key_send.at[index], key_parts.at[index], part_sem.at[index // 2], partner, 7)
        put(value_send.at[index], value_parts.at[index], value_sem.at[index // 2], partner, 8)

    def arrive_rows(index):
        for k in range(2):
            block = block_of(index, k)
            arrive(rows.at[block], row_sem.at[block], f"wfwd{index}")

    project(0)
    pass_rows(3)
    arrive_rows(1)
    project(1)
    project(2)
    shifted = (
        lax.broadcasted_iota(jnp.int32, (tokens, 128), 0) + 64
        == lax.broadcasted_iota(jnp.int32, (tokens, 128), 1)
    )
    for s in range(8):
        column = jnp.sum(jnp.where(shifted, row_data[s], 0.0), axis=1, keepdims=True)
        doc_wide[s * tokens:(s + 1) * tokens, :] = jnp.broadcast_to(column, (tokens, 128))
    query_index = lax.broadcasted_iota(jnp.int32, (length, length), 0)
    key_index = lax.broadcasted_iota(jnp.int32, (length, length), 1)
    doc_column = doc_wide[:, :1]
    doc_row = jnp.sum(jnp.where(query_index == key_index, doc_column, 0.0), axis=0, keepdims=True)
    forward(home_head, 1 - parity, y, 1)

    @pl.when(core != plane)
    def _():
        forward(home_head, 1 - parity, 1 - y, 1)

    arrive_rows(3)
    project(3)

    @pl.when(core == plane)
    def _():
        forward(home_head, 1 - parity, 1 - y, 1)

    arrive(tables, table_sem, "wtable")
    arrive_own(home_head)

    def home_part(half, c):
        total = None
        for index in range(4):
            at = place_rows(index * 2 + c)
            part = jnp.dot(normed[half, :, at], wide[home_head, at, :], preferred_element_type=jnp.float32)
            total = part if total is None else total + part
        return total

    for half in range(2):
        home[half] = home_part(half, core)
    arrive_side(home_head)

    factor = HEAD_DIM ** (-0.5)
    head = y * 2 + upper
    out_columns = pl.ds(pl.multiple_of(head * head_cols, 128), head_cols)
    half_rows = length // 2
    for half in range(2):
        whole = home[half] + home_part(half, 1 - core)
        arrive(key_parts.at[2 * half:2 * half + 2], part_sem.at[half], f"wpart{half}")
        arrive(value_parts.at[2 * half:2 * half + 2], value_sem.at[half], f"wpart{half}")
        for index in range(2 * half, 2 * half + 2):
            for k in range(2):
                block = pl.ds(pl.multiple_of(block_of(index, k) * tokens, 16), tokens)
                near_rows = slice(k * tokens, (k + 1) * tokens)
                spot = (index % 2 * 2 + k) * tokens
                raw_keys = whole[spot:spot + tokens, :HEAD_DIM] + key_parts[index, near_rows, :]
                raw_values = whole[spot:spot + tokens, HEAD_DIM:] + value_parts[index, near_rows, :].astype(jnp.float32)
                key_heads[block, :] = (
                    raw_keys * tables[0, block, :] + pltpu.roll(raw_keys, HEAD_DIM // 2, 1) * tables[1, block, :]
                ).astype(jnp.bfloat16)
                value_heads[block, :] = raw_values.astype(jnp.bfloat16)
        first, last = half * half_rows, (half + 1) * half_rows
        arrive(query_rows.at[first:last], query_sem.at[half], f"wq{half}")
        allowed = (
            lax.broadcasted_iota(jnp.int32, (half_rows, last), 1)
            <= first + lax.broadcasted_iota(jnp.int32, (half_rows, last), 0)
        ) & (doc_row[:, :last] == doc_wide[first:last, :1])
        for g in range(group_size):
            cols = slice(g * HEAD_DIM, (g + 1) * HEAD_DIM)
            scores = lax.dot_general(
                query_rows[first:last, cols], key_heads[:last, :], (((1,), (1,)), ((), ())),
                preferred_element_type=jnp.float32,
            ) * factor
            scores = jnp.where(allowed, scores, MASKED)
            highest = jnp.max(scores, axis=-1, keepdims=True)
            exponent = jnp.exp(scores - highest)
            weights = (exponent / jnp.sum(exponent, axis=-1, keepdims=True)).astype(jnp.bfloat16)
            mixed[half, :, cols] = jnp.dot(
                weights, value_heads[:last, :], preferred_element_type=jnp.float32
            ).astype(jnp.bfloat16)
        for k in range(4):
            to_sp = half * 4 + k
            send(
                mixed.at[half, k * tokens:(k + 1) * tokens], out.at[plane, 0, :, out_columns], out_sem,
                {"groups": core, "sp": to_sp, "fsdp": parity}, 9,
                (core == plane) & (sp == to_sp) & (core == parity),
            )
    def sent(ref, index):
        pltpu.make_async_copy(ref, ref, send_sem.at[index]).wait()

    with scope("wsend"):
        sent(wide.at[0], 0)
        sent(wide.at[1, :6 * features], 1)
        sent(gain_rows.at[:7], 3)
        sent(rows.at[:4], 6)
        sent(key_send, 7)
        sent(value_send, 8)
        for count in (7, 8):
            @pl.when(own_any if count == 7 else jnp.logical_not(own_any))
            def _(count=count):
                sent(rows.at[:count - 4], 2)
                sent(row_data.at[:count], 4)
                sent(query_rows.at[:count * tokens], 5)
                sent(query_rows.at[:count * tokens], 9)
    arrive(out, out_sem, "wout")


def fused(mesh, hiddens, queries, documents, gains, keys, values):
    sp = mesh.shape["sp"]
    tokens, features = hiddens[0].shape[1], keys[0].shape[0]
    kv_heads = keys[0].shape[1] // HEAD_DIM
    head_cols = queries[0].shape[2] // kv_heads
    length = sp * tokens
    half_dim = HEAD_DIM // 2
    frequency = ROPE_BASE ** (-2.0 * np.arange(half_dim) / HEAD_DIM)
    angles = np.arange(length)[:, None] * frequency[None, :]
    cosines = np.concatenate([np.cos(angles), np.cos(angles)], axis=1).astype(np.float32)
    sines = np.concatenate([-np.sin(angles), np.sin(angles)], axis=1).astype(np.float32)
    dma = pltpu.SemaphoreType.DMA
    bf16, f32 = jnp.bfloat16, jnp.float32
    out = pl.pallas_call(
        fused_kernel,
        out_shape=pltpu.VMEM((2, 1, tokens, queries[0].shape[2]), bf16),
        in_specs=[pl.BlockSpec(memory_space=pl.ANY)] * 13,
        out_specs=pl.BlockSpec(memory_space=pltpu.VMEM),
        scratch_shapes=[
            pltpu.VMEM((features,), bf16),
            pltpu.VMEM((features,), bf16),
            pltpu.VMEM((2, 1, tokens), jnp.int32),
            pltpu.VMEM((2,) + hiddens[0].shape[1:], bf16),
            pltpu.VMEM((sp, tokens, 8 * features), bf16),
            pltpu.VMEM((2, 8 * features, 2 * HEAD_DIM), bf16),
            pltpu.VMEM((2, 4 * tokens, 8 * features), bf16),
            pltpu.VMEM((1, features), f32),
            pltpu.VMEM((8, 1, features), f32),
            pltpu.VMEM((2, 1, 128), f32),
            pltpu.VMEM((sp, 1, 128), f32),
            pltpu.VMEM((length, head_cols), bf16),
            pltpu.VMEM((length, 128), f32),
            pltpu.VMEM((4, 2 * tokens, HEAD_DIM), f32),
            pltpu.VMEM((4, 2 * tokens, HEAD_DIM), bf16),
            pltpu.VMEM((4, 2 * tokens, HEAD_DIM), f32),
            pltpu.VMEM((4, 2 * tokens, HEAD_DIM), bf16),
            pltpu.VMEM((2, length // 2, 2 * HEAD_DIM), f32),
            pltpu.VMEM((length, HEAD_DIM), bf16),
            pltpu.VMEM((length, HEAD_DIM), bf16),
            pltpu.VMEM((2, length // 2, head_cols), bf16),
            pltpu.VMEM((2, length, HEAD_DIM), f32),
            pltpu.SemaphoreType.REGULAR((4,)),
            dma((4,)),
            dma(()),
            dma(()),
            dma((10,)),
            dma((sp,)),
            dma((2, 4)),
            dma((2,)),
            dma(()),
            dma((2,)),
            dma((2,)),
            dma((2,)),
            dma((2,)),
            dma(()),
        ],
        compiler_params=pltpu.CompilerParams(collective_id=0, has_side_effects=True),
        name="fused",
    )(
        *hiddens, *queries, *keys, *values, np.stack([cosines, sines]),
        *gains, *documents,
    )
    return out[0], out[1]


def per_device(
    mesh,
    policy_hidden,
    policy_queries,
    policy_documents,
    policy_gain,
    policy_key_weight,
    policy_value_weight,
    frozen_hidden,
    frozen_queries,
    frozen_documents,
    frozen_gain,
    frozen_key_weight,
    frozen_value_weight,
):
    if fits(mesh, policy_hidden, policy_queries, policy_key_weight):
        return fused(
            mesh,
            (policy_hidden, frozen_hidden),
            (policy_queries, frozen_queries),
            (policy_documents, frozen_documents),
            (policy_gain, frozen_gain),
            (policy_key_weight, frozen_key_weight),
            (policy_value_weight, frozen_value_weight),
        )
    policy_mixed = run_model(
        policy_hidden,
        policy_queries,
        policy_documents,
        policy_gain,
        policy_key_weight,
        policy_value_weight,
    )
    frozen_mixed = run_model(
        frozen_hidden,
        frozen_queries,
        frozen_documents,
        frozen_gain,
        frozen_key_weight,
        frozen_value_weight,
    )
    return (policy_mixed, frozen_mixed)


def solution(mesh):
    return jax.shard_map(
        functools.partial(per_device, mesh),
        mesh=mesh,
        in_specs=(
            P(("groups", "fsdp"), "sp", None),
            P(("groups", "fsdp"), "sp", None),
            P(("groups", "fsdp"), "sp"),
            P(("sp", "fsdp")),
            P(("sp", "fsdp"), None),
            P(("sp", "fsdp"), None),
            P(("groups", "fsdp"), "sp", None),
            P(("groups", "fsdp"), "sp", None),
            P(("groups", "fsdp"), "sp"),
            P(("sp", "fsdp")),
            P(("sp", "fsdp"), None),
            P(("sp", "fsdp"), None),
        ),
        out_specs=(P(("groups", "fsdp"), "sp", None), P(("groups", "fsdp"), "sp", None)),
        check_vma=False,
    )
```

```python
import contextlib
import functools

import jax
import jax.numpy as jnp
import numpy as np
from jax import lax
from jax.experimental import pallas as pl
from jax.experimental.pallas import tpu as pltpu
from jax.sharding import PartitionSpec as P

HEAD_DIM = 128


EPS = 1e-05
ROPE_BASE = 500000.0
MASKED = -1e30


def rotate(raw_keys, positions):
    half_dim = HEAD_DIM // 2
    frequency = jnp.exp(
        -jnp.log(ROPE_BASE) * jnp.arange(half_dim, dtype=jnp.float32) * 2.0 / HEAD_DIM
    )
    angles = positions.astype(jnp.float32)[:, None] * frequency[None, :]
    cosines = jnp.cos(angles)[:, None, :]
    sines = jnp.sin(angles)[:, None, :]
    front_half = raw_keys[..., :half_dim]
    back_half = raw_keys[..., half_dim:]
    return jnp.concatenate(
        [front_half * cosines - back_half * sines, back_half * cosines + front_half * sines],
        axis=-1,
    )


def project(hidden, gain, key_weight, value_weight):
    tokens = hidden.shape[1]
    widened = hidden[0].astype(jnp.float32)
    inverse = lax.rsqrt(jnp.mean(widened * widened, axis=-1, keepdims=True) + EPS)
    scaled = widened * inverse
    gain_rows = lax.all_gather(gain, ("sp", "fsdp"), axis=0, tiled=True)
    key_rows = lax.all_gather(key_weight, ("sp", "fsdp"), axis=0, tiled=True)
    value_rows = lax.all_gather(value_weight, ("sp", "fsdp"), axis=0, tiled=True)
    normed = (scaled * gain_rows.astype(jnp.float32)[None, :]).astype(jnp.bfloat16)
    raw_keys = jnp.dot(normed, key_rows, preferred_element_type=jnp.float32)
    raw_values = jnp.dot(normed, value_rows, preferred_element_type=jnp.float32)
    positions = lax.axis_index("sp") * tokens + jnp.arange(tokens, dtype=jnp.int32)
    key_heads = rotate(raw_keys.reshape(tokens, -1, HEAD_DIM), positions).astype(jnp.bfloat16)
    value_heads = raw_values.astype(jnp.bfloat16).reshape(tokens, -1, HEAD_DIM)
    return (key_heads, value_heads)


def attend(queries, key_heads, value_heads, documents):
    length = queries.shape[0]
    head_count = queries.shape[1]
    block_rows = min(512, length)
    margin = min(512, length // 2)
    window = block_rows + margin
    factor = HEAD_DIM ** (-0.5)
    offsets = jnp.arange(block_rows, dtype=jnp.int32)
    window_offsets = jnp.arange(window, dtype=jnp.int32)
    padding = jnp.zeros((margin, head_count, HEAD_DIM), jnp.bfloat16)
    padded_keys = jnp.concatenate([padding, key_heads], axis=0)
    padded_values = jnp.concatenate([padding, value_heads], axis=0)
    padded_docs = jnp.concatenate([jnp.full((margin,), -1, jnp.int32), documents], axis=0)

    def one_block(block_index):
        first = block_index * block_rows
        query_block = lax.dynamic_slice_in_dim(queries, first, block_rows, 0)
        query_docs = lax.dynamic_slice_in_dim(documents, first, block_rows, 0)
        query_positions = first + offsets
        key_block = lax.dynamic_slice_in_dim(padded_keys, first, window, 0)
        value_block = lax.dynamic_slice_in_dim(padded_values, first, window, 0)
        key_docs = lax.dynamic_slice_in_dim(padded_docs, first, window, 0)
        key_positions = first - margin + window_offsets
        allowed = (key_positions[None, :] <= query_positions[:, None]) & (
            key_docs[None, :] == query_docs[:, None]
        )
        scores = (
            jnp.einsum("qnd,knd->nqk", query_block, key_block, preferred_element_type=jnp.float32)
            * factor
        )
        scores = jnp.where(allowed[None], scores, MASKED)
        highest = jnp.max(scores, axis=-1, keepdims=True)
        exponent = jnp.where(allowed[None], jnp.exp(scores - highest), 0.0)
        weights = (exponent / jnp.sum(exponent, axis=-1, keepdims=True)).astype(jnp.bfloat16)
        blended = jnp.einsum(
            "nqk,knd->qnd", weights, value_block, preferred_element_type=jnp.float32
        )
        return blended.astype(jnp.bfloat16)

    blocks = lax.map(one_block, jnp.arange(length // block_rows, dtype=jnp.int32))
    return blocks.reshape(length, head_count, HEAD_DIM)


def run_model(hidden, queries, documents, gain, key_weight, value_weight):
    tokens = hidden.shape[1]
    head_count = queries.shape[2] // HEAD_DIM
    query_local = queries[0].reshape(tokens, head_count, HEAD_DIM)
    every_doc = lax.all_gather(documents[0], "sp", axis=0, tiled=True)
    key_heads, value_heads = project(hidden, gain, key_weight, value_weight)
    group_size = head_count // key_heads.shape[1]
    wide_keys = jnp.repeat(key_heads, group_size, axis=1)
    wide_values = jnp.repeat(value_heads, group_size, axis=1)
    query_spread, key_spread, value_spread = (
        lax.all_to_all(query_local, "sp", split_axis=1, concat_axis=0, tiled=True),
        lax.all_to_all(wide_keys, "sp", split_axis=1, concat_axis=0, tiled=True),
        lax.all_to_all(wide_values, "sp", split_axis=1, concat_axis=0, tiled=True),
    )
    mixed = attend(query_spread, key_spread, value_spread, every_doc)
    returned = lax.all_to_all(mixed, "sp", split_axis=0, concat_axis=1, tiled=True)
    return returned.reshape(1, tokens, head_count * HEAD_DIM)


MESH = pl.DeviceIdType.MESH
TRACE = False


def fits(mesh, hidden, queries, key_weight):
    sp, cores = mesh.shape["sp"], mesh.shape["fsdp"]
    tokens = hidden.shape[1]
    kv_heads = key_weight.shape[1] // HEAD_DIM
    return (
        cores == 2
        and mesh.shape["groups"] == 2
        and sp == 8
        and kv_heads == 4
        and queries.shape[2] % (kv_heads * HEAD_DIM) == 0
        and key_weight.shape[0] % 128 == 0
        and hidden.shape[2] == key_weight.shape[0] * sp * cores
        and tokens % 16 == 0
        and tokens <= 64
    )


def fused_kernel(
    hidden0, hidden1, queries0, queries1, key0, key1, value0, value1, table,
    gain0, gain1, documents0, documents1,
    out,
    gain_raw0, gain_raw1, doc_raw, near, rows, wide, normed, gain_send, gain_rows, row_send, row_data, query_rows, doc_wide,
    key_send, value_send, key_parts, value_parts, home, key_heads, value_heads, mixed, tables,
    ready, raw_sem, near_sem, table_sem, send_sem, row_sem, wide_sem, side_sem, gain_sem, data_sem, query_sem, part_sem, value_sem, out_sem,
):
    hiddens, queries = (hidden0, hidden1), (queries0, queries1)
    keys, values = (key0, key1), (value0, value1)
    tokens, features = hidden0.shape[1], key0.shape[0]
    slab = 8 * features
    head_cols = query_rows.shape[1]
    group_size = head_cols // HEAD_DIM
    length = query_rows.shape[0]
    sp, core, plane = lax.axis_index("sp"), lax.axis_index("fsdp"), lax.axis_index("groups")
    z, y = sp // 2, sp % 2
    upper, parity = z // 2, z % 2
    near_z = z + 1 - 2 * parity
    far_z = lax.rem(z + 2, 4)

    def scope(name):
        return jax.named_scope(name) if TRACE else contextlib.nullcontext()

    inner = upper != parity
    greeted = 4 + jnp.where(inner, 1, 0)

    def greet(semaphore):
        for target in (
            {"sp": near_z * 2 + y}, {"sp": z * 2 + 1 - y}, {"groups": 1 - plane}, {"fsdp": 1 - core},
        ):
            pl.semaphore_signal(semaphore, inc=1, device_id=target, device_id_type=MESH)

        @pl.when(inner)
        def _():
            pl.semaphore_signal(semaphore, inc=1, device_id={"sp": (3 - z) * 2 + y}, device_id_type=MESH)

    barrier = pltpu.get_barrier_semaphore()
    greet(barrier)

    def place(zz, yy, cc):
        return (zz * 2 + yy) * 2 + cc

    def place_rows(index):
        return pl.ds(pl.multiple_of(index * features, 128), features)

    mine = place(parity, y, core)
    leads = core == plane

    def columns(half, b):
        return pl.ds(pl.multiple_of((half * 2 + b) * HEAD_DIM, HEAD_DIM), HEAD_DIM)

    for m in range(2):
        pltpu.make_async_copy(hiddens[m].at[0], near.at[m], near_sem).start()
    small = (
        (gain0, gain_raw0), (gain1, gain_raw1), (documents0, doc_raw.at[0]), (documents1, doc_raw.at[1]),
    )
    for index, (src, dst) in enumerate(small):
        pltpu.make_async_copy(src, dst, raw_sem.at[index]).start()
    with scope("wbar"):
        pl.semaphore_wait(barrier, greeted)
    greet(ready.at[0])

    def next_round(step):
        with scope(f"wround{step}"):
            pl.semaphore_wait(ready.at[step], greeted)
        if step < 2:
            greet(ready.at[step + 1])

    def put(src, dst, recv, target, sent, away=None):
        def start():
            pltpu.make_async_remote_copy(
                src_ref=src, dst_ref=dst, send_sem=send_sem.at[sent], recv_sem=recv,
                device_id=target, device_id_type=MESH,
            ).start()

        if away is None:
            start()
        else:
            pl.when(away)(start)

    def send(src, dst, recv, target, sent, own):
        put(src, dst, recv, target, sent, jnp.logical_not(own))

        @pl.when(own)
        def _():
            pltpu.make_async_copy(src, dst, recv).start()

    def put_weight(b, half, target, sent, recv, model, when=None):
        for index, weights in enumerate((keys, values)):
            cols = slice(index * HEAD_DIM, (index + 1) * HEAD_DIM)
            for m in range(2):
                put(
                    weights[m].at[:, columns(half, b)], wide.at[b, place_rows(mine), cols], recv,
                    target, sent, model == m if when is None else (model == m) & when,
                )

    def arrive(dst, recv, name):
        with scope(name):
            pltpu.make_async_copy(dst, dst, recv).wait()

    def lane(zz, yy):
        return zz * 2 + yy

    def forward(b, zz, yy):
        block = wide.at[b, place_rows(place(zz, yy, core))]
        arrive(block, wide_sem.at[b, lane(zz, yy)], ("wa" if b is away_head else "wh") + f"{1 if zz is parity else 0}{1 if yy is y else 0}")
        put(block, block, wide_sem.at[b, lane(zz, yy)], {"groups": 1 - plane}, 1, leads)
        put(block, block, side_sem.at[b], beside, 0)

    def arrive_own(b):
        arrive(wide.at[b, place_rows(mine)], wide_sem.at[b, lane(parity, y)], "wown")

    def arrive_side(b):
        arrive(wide.at[b, :4 * features], side_sem.at[b], "wside")

    across, beside, along = {"sp": z * 2 + 1 - y}, {"fsdp": 1 - core}, {"sp": near_z * 2 + y}
    beyond = {"sp": near_z * 2 + 1 - y}
    away_head, home_head = 1 - upper, upper

    own_lane = lane(parity, y)

    def put_weights(b, first):
        recv = wide_sem.at[b, own_lane]
        if first != 1:
            put_weight(b, 1 - y, across, 1, recv, parity, leads)
            put_weight(b, y, along, 1, recv, 1 - parity, leads)
            put_weight(b, y, beside, 0, side_sem.at[b], parity)
        if first != 0:
            put_weight(b, 1 - y, beyond, 1, recv, 1 - parity, leads)

    put_weights(away_head, 0)
    for m in range(2):
        @pl.when(parity == m)
        def _(m=m):
            for b in range(2):
                target = wide.at[b, place_rows(mine)]
                pltpu.make_async_copy(
                    keys[m].at[:, columns(y, b)], target.at[:, :HEAD_DIM], wide_sem.at[b, own_lane]
                ).start()
                pltpu.make_async_copy(
                    values[m].at[:, columns(y, b)], target.at[:, HEAD_DIM:], wide_sem.at[b, own_lane]
                ).start()

    pltpu.make_async_copy(table, tables, table_sem).start()
    pltpu.make_async_copy(near, near, near_sem).wait()

    def put_hidden(h, m):
        src = near.at[m, :, pl.ds(pl.multiple_of(h * slab, 128), slab)]
        put(src, rows.at[sp], row_sem.at[sp], {"sp": (2 * h + m) * 2 + y}, 2)

    put_hidden(upper, 1 - parity)
    pltpu.make_async_copy(
        near.at[parity, :, pl.ds(pl.multiple_of(upper * slab, 128), slab)], rows.at[sp], row_sem.at[sp]
    ).start()
    next_round(0)
    put_weights(away_head, 1)
    first_far = jnp.where(inner, 1 - upper, upper)
    put_hidden(1 - upper, first_far)
    for index, (src, dst) in enumerate(small):
        pltpu.make_async_copy(src, dst, raw_sem.at[index]).wait()
    square = (
        lax.broadcasted_iota(jnp.int32, (tokens, 128), 0)
        == lax.broadcasted_iota(jnp.int32, (tokens, 128), 1)
    )
    for m in range(2):
        gain_send[m] = (gain_raw0, gain_raw1)[m][...].astype(jnp.float32).reshape(1, -1)
        wide_row = near[m].astype(jnp.float32)
        inverse = lax.rsqrt(jnp.mean(wide_row * wide_row, axis=-1, keepdims=True) + EPS)
        row_send[m] = jnp.sum(jnp.where(square, inverse, 0.0), axis=0, keepdims=True)
        row_send[m, :, 64:64 + tokens] = doc_raw[m].astype(jnp.float32)
    next_round(1)
    put_hidden(1 - upper, 1 - first_far)
    for m in range(2):
        for yy in range(2):
            for cc in range(2):
                send(
                    gain_send.at[m], gain_rows.at[mine], gain_sem,
                    {"sp": (upper * 2 + m) * 2 + yy, "fsdp": cc}, 3, (parity == m) & (y == yy) & (core == cc),
                )
    next_round(2)
    token_rows = pl.ds(pl.multiple_of(sp * tokens, 16), tokens)
    for m in range(2):
        for yy in range(2):
            for h in range(2):
                to_sp = (2 * h + m) * 2 + yy
                send(row_send.at[m], row_data.at[sp], data_sem.at[upper], {"sp": to_sp}, 4, sp == to_sp)
    for m in range(2):
        for yy in range(2):
            for h in range(2):
                to_sp, head = (2 * h + m) * 2 + yy, yy * 2 + h
                send(
                    queries[m].at[0, :, head * head_cols:(head + 1) * head_cols],
                    query_rows.at[token_rows], query_sem.at[upper], {"sp": to_sp}, 5, sp == to_sp,
                )
    put_weights(home_head, 2)

    def pass_rows(step):
        from_z = order[step]
        block = from_z * 2 + y
        arrive(rows.at[block], row_sem.at[block], f"whid{step}")
        put(rows.at[block], rows.at[block], row_sem.at[block], across, 6)

    order = (z, near_z, 3 * (1 - upper), 2 - upper)
    def forward_all(b, *lanes):
        for zz, yy in lanes:
            forward(b, zz, yy)

    side_lane, next_lane, last_lane = (parity, 1 - y), (1 - parity, y), (1 - parity, 1 - y)
    follows = jnp.logical_not(leads)

    def led(b, *lanes):
        pl.when(leads)(lambda: forward_all(b, *lanes))

    def followed(b, *lanes):
        pl.when(follows)(lambda: forward_all(b, *lanes))

    pass_rows(0)
    led(away_head, side_lane, next_lane)
    pass_rows(1)
    led(away_head, last_lane)
    pl.when(follows)(lambda: pass_rows(2))
    followed(away_head, side_lane, next_lane, last_lane)
    pl.when(leads)(lambda: pass_rows(2))
    pass_rows(3)
    arrive(gain_rows, gain_sem, "wgain")
    arrive_own(away_head)
    arrive_side(away_head)
    gain_row = jnp.concatenate([gain_rows[s] for s in range(8)], axis=1)
    partner = {"sp": far_z * 2 + y}

    def block_of(half, side, k):
        return half * 4 + 2 * k + (y if side == 0 else 1 - y)

    def project(half, side):
        for k in range(2):
            s = block_of(half, side, k)
            scale = jnp.sum(jnp.where(square, row_data[s], 0.0), axis=1, keepdims=True)
            spot = (side * 2 + k) * tokens
            normed[half, spot:spot + tokens, :] = (
                rows[s].astype(jnp.float32) * scale * gain_row
            ).astype(jnp.bfloat16)
        spot = side * 2 * tokens
        part = jnp.dot(
            normed[half, spot:spot + 2 * tokens, :], wide[away_head], preferred_element_type=jnp.float32
        )
        index = half * 2 + side
        key_send[index] = part[:, :HEAD_DIM]
        value_send[index] = part[:, HEAD_DIM:].astype(jnp.bfloat16)
        put(key_send.at[index], key_parts.at[index], part_sem.at[half], partner, 7)
        put(value_send.at[index], value_parts.at[index], value_sem.at[half], partner, 8)

    def arrive_data(half):
        arrive(row_data.at[pl.ds(4 * half, 4)], data_sem.at[half], "wdata")

    def arrive_rows(half):
        for k in range(2):
            block = block_of(half, 1, k)
            arrive(rows.at[block], row_sem.at[block], "wfwd")

    arrive_data(upper)
    project(upper, 0)
    arrive_rows(upper)
    project(upper, 1)
    led(home_head, side_lane, next_lane)
    arrive_data(1 - upper)
    project(1 - upper, 0)
    led(home_head, last_lane)
    shifted = (
        lax.broadcasted_iota(jnp.int32, (tokens, 128), 0) + 64
        == lax.broadcasted_iota(jnp.int32, (tokens, 128), 1)
    )
    for s in range(8):
        column = jnp.sum(jnp.where(shifted, row_data[s], 0.0), axis=1, keepdims=True)
        doc_wide[s * tokens:(s + 1) * tokens, :] = jnp.broadcast_to(column, (tokens, 128))
    query_index = lax.broadcasted_iota(jnp.int32, (length, length), 0)
    key_index = lax.broadcasted_iota(jnp.int32, (length, length), 1)
    doc_column = doc_wide[:, :1]
    doc_row = jnp.sum(jnp.where(query_index == key_index, doc_column, 0.0), axis=0, keepdims=True)
    arrive_rows(1 - upper)
    project(1 - upper, 1)
    followed(home_head, side_lane, next_lane, last_lane)
    arrive(tables, table_sem, "wtable")
    arrive_own(home_head)

    def home_part(half, c):
        total = None
        for index in range(4):
            at = place_rows(index * 2 + c)
            part = jnp.dot(normed[half, :, at], wide[home_head, at, :], preferred_element_type=jnp.float32)
            total = part if total is None else total + part
        return total

    for half in range(2):
        home[half] = home_part(half, core)
    arrive_side(home_head)

    factor = HEAD_DIM ** (-0.5)
    head = y * 2 + upper
    out_columns = pl.ds(pl.multiple_of(head * head_cols, 128), head_cols)
    half_rows = length // 2
    for half in range(2):
        whole = home[half] + home_part(half, 1 - core)
        arrive(key_parts.at[2 * half:2 * half + 2], part_sem.at[half], f"wpart{half}")
        arrive(value_parts.at[2 * half:2 * half + 2], value_sem.at[half], f"wpart{half}")
        for index in range(2 * half, 2 * half + 2):
            for k in range(2):
                block = pl.ds(pl.multiple_of(block_of(half, index % 2, k) * tokens, 16), tokens)
                near_rows = slice(k * tokens, (k + 1) * tokens)
                spot = (index % 2 * 2 + k) * tokens
                raw_keys = whole[spot:spot + tokens, :HEAD_DIM] + key_parts[index, near_rows, :]
                raw_values = whole[spot:spot + tokens, HEAD_DIM:] + value_parts[index, near_rows, :].astype(jnp.float32)
                key_heads[block, :] = (
                    raw_keys * tables[0, block, :] + pltpu.roll(raw_keys, HEAD_DIM // 2, 1) * tables[1, block, :]
                ).astype(jnp.bfloat16)
                value_heads[block, :] = raw_values.astype(jnp.bfloat16)
        first, last = half * half_rows, (half + 1) * half_rows
        arrive(query_rows.at[first:last], query_sem.at[half], f"wq{half}")
        allowed = (
            lax.broadcasted_iota(jnp.int32, (half_rows, last), 1)
            <= first + lax.broadcasted_iota(jnp.int32, (half_rows, last), 0)
        ) & (doc_row[:, :last] == doc_wide[first:last, :1])
        for g in range(group_size):
            cols = slice(g * HEAD_DIM, (g + 1) * HEAD_DIM)
            scores = lax.dot_general(
                query_rows[first:last, cols], key_heads[:last, :], (((1,), (1,)), ((), ())),
                preferred_element_type=jnp.float32,
            ) * factor
            scores = jnp.where(allowed, scores, MASKED)
            highest = jnp.max(scores, axis=-1, keepdims=True)
            exponent = jnp.exp(scores - highest)
            weights = (exponent / jnp.sum(exponent, axis=-1, keepdims=True)).astype(jnp.bfloat16)
            mixed[half, :, cols] = jnp.dot(
                weights, value_heads[:last, :], preferred_element_type=jnp.float32
            ).astype(jnp.bfloat16)
        for k in range(4):
            to_sp = half * 4 + k
            send(
                mixed.at[half, k * tokens:(k + 1) * tokens], out.at[parity, 0, :, out_columns], out_sem,
                {"sp": to_sp}, 9, sp == to_sp,
            )
    def sent(ref, index):
        pltpu.make_async_copy(ref, ref, send_sem.at[index]).wait()

    with scope("wsend"):
        sent(wide.at[0], 0)

        @pl.when(leads)
        def _():
            sent(wide.at[:, :6 * features], 1)

        sent(rows.at[:3], 2)
        sent(gain_rows.at[:7], 3)
        sent(row_data.at[:7], 4)
        sent(query_rows.at[:7 * tokens], 5)
        sent(rows.at[:4], 6)
        sent(key_send, 7)
        sent(value_send, 8)
        sent(query_rows.at[:7 * tokens], 9)
    arrive(out, out_sem, "wout")


def fused(mesh, hiddens, queries, documents, gains, keys, values):
    sp = mesh.shape["sp"]
    tokens, features = hiddens[0].shape[1], keys[0].shape[0]
    kv_heads = keys[0].shape[1] // HEAD_DIM
    head_cols = queries[0].shape[2] // kv_heads
    length = sp * tokens
    half_dim = HEAD_DIM // 2
    frequency = ROPE_BASE ** (-2.0 * np.arange(half_dim) / HEAD_DIM)
    angles = np.arange(length)[:, None] * frequency[None, :]
    cosines = np.concatenate([np.cos(angles), np.cos(angles)], axis=1).astype(np.float32)
    sines = np.concatenate([-np.sin(angles), np.sin(angles)], axis=1).astype(np.float32)
    dma = pltpu.SemaphoreType.DMA
    bf16, f32 = jnp.bfloat16, jnp.float32
    out = pl.pallas_call(
        fused_kernel,
        out_shape=pltpu.VMEM((2, 1, tokens, queries[0].shape[2]), bf16),
        in_specs=[pl.BlockSpec(memory_space=pl.ANY)] * 13,
        out_specs=pl.BlockSpec(memory_space=pltpu.VMEM),
        scratch_shapes=[
            pltpu.VMEM((features,), bf16),
            pltpu.VMEM((features,), bf16),
            pltpu.VMEM((2, 1, tokens), jnp.int32),
            pltpu.VMEM((2,) + hiddens[0].shape[1:], bf16),
            pltpu.VMEM((sp, tokens, 8 * features), bf16),
            pltpu.VMEM((2, 8 * features, 2 * HEAD_DIM), bf16),
            pltpu.VMEM((2, 4 * tokens, 8 * features), bf16),
            pltpu.VMEM((2, 1, features), f32),
            pltpu.VMEM((8, 1, features), f32),
            pltpu.VMEM((2, 1, 128), f32),
            pltpu.VMEM((sp, 1, 128), f32),
            pltpu.VMEM((length, head_cols), bf16),
            pltpu.VMEM((length, 128), f32),
            pltpu.VMEM((4, 2 * tokens, HEAD_DIM), f32),
            pltpu.VMEM((4, 2 * tokens, HEAD_DIM), bf16),
            pltpu.VMEM((4, 2 * tokens, HEAD_DIM), f32),
            pltpu.VMEM((4, 2 * tokens, HEAD_DIM), bf16),
            pltpu.VMEM((2, length // 2, 2 * HEAD_DIM), f32),
            pltpu.VMEM((length, HEAD_DIM), bf16),
            pltpu.VMEM((length, HEAD_DIM), bf16),
            pltpu.VMEM((2, length // 2, head_cols), bf16),
            pltpu.VMEM((2, length, HEAD_DIM), f32),
            pltpu.SemaphoreType.REGULAR((3,)),
            dma((4,)),
            dma(()),
            dma(()),
            dma((10,)),
            dma((sp,)),
            dma((2, 4)),
            dma((2,)),
            dma(()),
            dma((2,)),
            dma((2,)),
            dma((2,)),
            dma((2,)),
            dma(()),
        ],
        compiler_params=pltpu.CompilerParams(collective_id=0, has_side_effects=True),
        name="fused",
    )(
        *hiddens, *queries, *keys, *values, np.stack([cosines, sines]),
        *gains, *documents,
    )
    return out[0], out[1]


def per_device(
    mesh,
    policy_hidden,
    policy_queries,
    policy_documents,
    policy_gain,
    policy_key_weight,
    policy_value_weight,
    frozen_hidden,
    frozen_queries,
    frozen_documents,
    frozen_gain,
    frozen_key_weight,
    frozen_value_weight,
):
    if fits(mesh, policy_hidden, policy_queries, policy_key_weight):
        return fused(
            mesh,
            (policy_hidden, frozen_hidden),
            (policy_queries, frozen_queries),
            (policy_documents, frozen_documents),
            (policy_gain, frozen_gain),
            (policy_key_weight, frozen_key_weight),
            (policy_value_weight, frozen_value_weight),
        )
    policy_mixed = run_model(
        policy_hidden,
        policy_queries,
        policy_documents,
        policy_gain,
        policy_key_weight,
        policy_value_weight,
    )
    frozen_mixed = run_model(
        frozen_hidden,
        frozen_queries,
        frozen_documents,
        frozen_gain,
        frozen_key_weight,
        frozen_value_weight,
    )
    return (policy_mixed, frozen_mixed)


def solution(mesh):
    return jax.shard_map(
        functools.partial(per_device, mesh),
        mesh=mesh,
        in_specs=(
            P(("groups", "fsdp"), "sp", None),
            P(("groups", "fsdp"), "sp", None),
            P(("groups", "fsdp"), "sp"),
            P(("sp", "fsdp")),
            P(("sp", "fsdp"), None),
            P(("sp", "fsdp"), None),
            P(("groups", "fsdp"), "sp", None),
            P(("groups", "fsdp"), "sp", None),
            P(("groups", "fsdp"), "sp"),
            P(("sp", "fsdp")),
            P(("sp", "fsdp"), None),
            P(("sp", "fsdp"), None),
        ),
        out_specs=(P(("groups", "fsdp"), "sp", None), P(("groups", "fsdp"), "sp", None)),
        check_vma=False,
    )
```

```python
import contextlib
import functools

import jax
import jax.numpy as jnp
import numpy as np
from jax import lax
from jax.experimental import pallas as pl
from jax.experimental.pallas import tpu as pltpu
from jax.sharding import PartitionSpec as P

HEAD_DIM = 128


EPS = 1e-05
ROPE_BASE = 500000.0
MASKED = -1e30


def rotate(raw_keys, positions):
    half_dim = HEAD_DIM // 2
    frequency = jnp.exp(
        -jnp.log(ROPE_BASE) * jnp.arange(half_dim, dtype=jnp.float32) * 2.0 / HEAD_DIM
    )
    angles = positions.astype(jnp.float32)[:, None] * frequency[None, :]
    cosines = jnp.cos(angles)[:, None, :]
    sines = jnp.sin(angles)[:, None, :]
    front_half = raw_keys[..., :half_dim]
    back_half = raw_keys[..., half_dim:]
    return jnp.concatenate(
        [front_half * cosines - back_half * sines, back_half * cosines + front_half * sines],
        axis=-1,
    )


def project(hidden, gain, key_weight, value_weight):
    tokens = hidden.shape[1]
    widened = hidden[0].astype(jnp.float32)
    inverse = lax.rsqrt(jnp.mean(widened * widened, axis=-1, keepdims=True) + EPS)
    scaled = widened * inverse
    gain_rows = lax.all_gather(gain, ("sp", "fsdp"), axis=0, tiled=True)
    key_rows = lax.all_gather(key_weight, ("sp", "fsdp"), axis=0, tiled=True)
    value_rows = lax.all_gather(value_weight, ("sp", "fsdp"), axis=0, tiled=True)
    normed = (scaled * gain_rows.astype(jnp.float32)[None, :]).astype(jnp.bfloat16)
    raw_keys = jnp.dot(normed, key_rows, preferred_element_type=jnp.float32)
    raw_values = jnp.dot(normed, value_rows, preferred_element_type=jnp.float32)
    positions = lax.axis_index("sp") * tokens + jnp.arange(tokens, dtype=jnp.int32)
    key_heads = rotate(raw_keys.reshape(tokens, -1, HEAD_DIM), positions).astype(jnp.bfloat16)
    value_heads = raw_values.astype(jnp.bfloat16).reshape(tokens, -1, HEAD_DIM)
    return (key_heads, value_heads)


def attend(queries, key_heads, value_heads, documents):
    length = queries.shape[0]
    head_count = queries.shape[1]
    block_rows = min(512, length)
    margin = min(512, length // 2)
    window = block_rows + margin
    factor = HEAD_DIM ** (-0.5)
    offsets = jnp.arange(block_rows, dtype=jnp.int32)
    window_offsets = jnp.arange(window, dtype=jnp.int32)
    padding = jnp.zeros((margin, head_count, HEAD_DIM), jnp.bfloat16)
    padded_keys = jnp.concatenate([padding, key_heads], axis=0)
    padded_values = jnp.concatenate([padding, value_heads], axis=0)
    padded_docs = jnp.concatenate([jnp.full((margin,), -1, jnp.int32), documents], axis=0)

    def one_block(block_index):
        first = block_index * block_rows
        query_block = lax.dynamic_slice_in_dim(queries, first, block_rows, 0)
        query_docs = lax.dynamic_slice_in_dim(documents, first, block_rows, 0)
        query_positions = first + offsets
        key_block = lax.dynamic_slice_in_dim(padded_keys, first, window, 0)
        value_block = lax.dynamic_slice_in_dim(padded_values, first, window, 0)
        key_docs = lax.dynamic_slice_in_dim(padded_docs, first, window, 0)
        key_positions = first - margin + window_offsets
        allowed = (key_positions[None, :] <= query_positions[:, None]) & (
            key_docs[None, :] == query_docs[:, None]
        )
        scores = (
            jnp.einsum("qnd,knd->nqk", query_block, key_block, preferred_element_type=jnp.float32)
            * factor
        )
        scores = jnp.where(allowed[None], scores, MASKED)
        highest = jnp.max(scores, axis=-1, keepdims=True)
        exponent = jnp.where(allowed[None], jnp.exp(scores - highest), 0.0)
        weights = (exponent / jnp.sum(exponent, axis=-1, keepdims=True)).astype(jnp.bfloat16)
        blended = jnp.einsum(
            "nqk,knd->qnd", weights, value_block, preferred_element_type=jnp.float32
        )
        return blended.astype(jnp.bfloat16)

    blocks = lax.map(one_block, jnp.arange(length // block_rows, dtype=jnp.int32))
    return blocks.reshape(length, head_count, HEAD_DIM)


def run_model(hidden, queries, documents, gain, key_weight, value_weight):
    tokens = hidden.shape[1]
    head_count = queries.shape[2] // HEAD_DIM
    query_local = queries[0].reshape(tokens, head_count, HEAD_DIM)
    every_doc = lax.all_gather(documents[0], "sp", axis=0, tiled=True)
    key_heads, value_heads = project(hidden, gain, key_weight, value_weight)
    group_size = head_count // key_heads.shape[1]
    wide_keys = jnp.repeat(key_heads, group_size, axis=1)
    wide_values = jnp.repeat(value_heads, group_size, axis=1)
    query_spread, key_spread, value_spread = (
        lax.all_to_all(query_local, "sp", split_axis=1, concat_axis=0, tiled=True),
        lax.all_to_all(wide_keys, "sp", split_axis=1, concat_axis=0, tiled=True),
        lax.all_to_all(wide_values, "sp", split_axis=1, concat_axis=0, tiled=True),
    )
    mixed = attend(query_spread, key_spread, value_spread, every_doc)
    returned = lax.all_to_all(mixed, "sp", split_axis=0, concat_axis=1, tiled=True)
    return returned.reshape(1, tokens, head_count * HEAD_DIM)


MESH = pl.DeviceIdType.MESH
TRACE = False


def fits(mesh, hidden, queries, key_weight):
    sp, cores = mesh.shape["sp"], mesh.shape["fsdp"]
    tokens = hidden.shape[1]
    kv_heads = key_weight.shape[1] // HEAD_DIM
    return (
        cores == 2
        and mesh.shape["groups"] == 2
        and sp == 8
        and kv_heads == 4
        and queries.shape[2] % (kv_heads * HEAD_DIM) == 0
        and key_weight.shape[0] % 128 == 0
        and hidden.shape[2] == key_weight.shape[0] * sp * cores
        and tokens % 16 == 0
        and tokens <= 64
    )


def fused_kernel(
    hidden0, hidden1, queries0, queries1, key0, key1, value0, value1, table,
    gain0, gain1, documents0, documents1,
    out,
    gain_raw0, gain_raw1, doc_raw, near, rows, wide, normed, gain_send, gain_rows, row_send, row_data, query_rows, doc_wide,
    key_send, value_send, key_parts, value_parts, home, key_heads, value_heads, mixed, tables,
    ready, raw_sem, near_sem, table_sem, send_sem, row_sem, wide_sem, side_sem, gain_sem, data_sem, query_sem, part_sem, value_sem, out_sem,
):
    hiddens, queries = (hidden0, hidden1), (queries0, queries1)
    keys, values = (key0, key1), (value0, value1)
    tokens, features = hidden0.shape[1], key0.shape[0]
    slab = 8 * features
    head_cols = query_rows.shape[1]
    group_size = head_cols // HEAD_DIM
    length = query_rows.shape[0]
    sp, core, plane = lax.axis_index("sp"), lax.axis_index("fsdp"), lax.axis_index("groups")
    z, y = sp // 2, sp % 2
    upper, parity = z // 2, z % 2
    near_z = z + 1 - 2 * parity
    far_z = lax.rem(z + 2, 4)

    def scope(name):
        return jax.named_scope(name) if TRACE else contextlib.nullcontext()

    inner = upper != parity
    greeted = 4 + jnp.where(inner, 1, 0)

    def greet(semaphore):
        for target in (
            {"sp": near_z * 2 + y}, {"sp": z * 2 + 1 - y}, {"groups": 1 - plane}, {"fsdp": 1 - core},
        ):
            pl.semaphore_signal(semaphore, inc=1, device_id=target, device_id_type=MESH)

        @pl.when(inner)
        def _():
            pl.semaphore_signal(semaphore, inc=1, device_id={"sp": (3 - z) * 2 + y}, device_id_type=MESH)

    barrier = pltpu.get_barrier_semaphore()
    greet(barrier)

    def place(zz, yy, cc):
        return (zz * 2 + yy) * 2 + cc

    def place_rows(index):
        return pl.ds(pl.multiple_of(index * features, 128), features)

    mine = place(parity, y, core)
    leads, follows = core == plane, core != plane

    def columns(half, b):
        return pl.ds(pl.multiple_of((half * 2 + b) * HEAD_DIM, HEAD_DIM), HEAD_DIM)

    for m in range(2):
        pltpu.make_async_copy(hiddens[m].at[0], near.at[m], near_sem).start()
    small = (
        (gain0, gain_raw0), (gain1, gain_raw1), (documents0, doc_raw.at[0]), (documents1, doc_raw.at[1]),
    )
    for index, (src, dst) in enumerate(small):
        pltpu.make_async_copy(src, dst, raw_sem.at[index]).start()
    with scope("wbar"):
        pl.semaphore_wait(barrier, greeted)
    greet(ready.at[0])

    def next_round(step):
        with scope(f"wround{step}"):
            pl.semaphore_wait(ready.at[step], greeted)
        if step < 2:
            greet(ready.at[step + 1])

    def put(src, dst, recv, target, sent, away=None):
        def start():
            pltpu.make_async_remote_copy(
                src_ref=src, dst_ref=dst, send_sem=send_sem.at[sent], recv_sem=recv,
                device_id=target, device_id_type=MESH,
            ).start()

        if away is None:
            start()
        else:
            pl.when(away)(start)

    def send(src, dst, recv, target, sent, own):
        put(src, dst, recv, target, sent, jnp.logical_not(own))

        @pl.when(own)
        def _():
            pltpu.make_async_copy(src, dst, recv).start()

    def put_weight(b, half, target, sent, recv, model, when=None):
        for index, weights in enumerate((keys, values)):
            cols = slice(index * HEAD_DIM, (index + 1) * HEAD_DIM)
            for m in range(2):
                put(
                    weights[m].at[:, columns(half, b)], wide.at[b, place_rows(mine), cols], recv,
                    target, sent, model == m if when is None else (model == m) & when,
                )

    def arrive(dst, recv, name):
        with scope(name):
            pltpu.make_async_copy(dst, dst, recv).wait()

    def lane(zz, yy):
        return zz * 2 + yy

    def forward(b, zz, yy, onward):
        block = wide.at[b, place_rows(place(zz, yy, core))]
        arrive(block, wide_sem.at[b, lane(zz, yy)], ("wa" if b is away_head else "wh") + f"{1 if zz is parity else 0}{1 if yy is y else 0}")
        if onward:
            put(block, block, wide_sem.at[b, lane(zz, yy)], {"groups": 1 - plane}, 1)
        put(block, block, side_sem.at[b], beside, 0)

    def arrive_own(b):
        arrive(wide.at[b, place_rows(mine)], wide_sem.at[b, lane(parity, y)], "wown")

    def arrive_side(b):
        arrive(wide.at[b, :4 * features], side_sem.at[b], "wside")

    across, beside, along = {"sp": z * 2 + 1 - y}, {"fsdp": 1 - core}, {"sp": near_z * 2 + y}
    beyond = {"sp": near_z * 2 + 1 - y}
    away_head, home_head = 1 - upper, upper

    own_lane = lane(parity, y)

    def put_weights(b, lead, first):
        recv = wide_sem.at[b, own_lane]
        if first != 1:
            put_weight(b, 1 - y, across, 1, recv, parity, lead)
            put_weight(b, y, along, 1, recv, 1 - parity, lead)
            put_weight(b, y, beside, 0, side_sem.at[b], parity)
        if first != 0:
            put_weight(b, 1 - y, beyond, 1, recv, 1 - parity, lead)

    put_weights(away_head, leads, 0)
    for m in range(2):
        @pl.when(parity == m)
        def _(m=m):
            for b in range(2):
                target = wide.at[b, place_rows(mine)]
                pltpu.make_async_copy(
                    keys[m].at[:, columns(y, b)], target.at[:, :HEAD_DIM], wide_sem.at[b, own_lane]
                ).start()
                pltpu.make_async_copy(
                    values[m].at[:, columns(y, b)], target.at[:, HEAD_DIM:], wide_sem.at[b, own_lane]
                ).start()

    pltpu.make_async_copy(table, tables, table_sem).start()
    pltpu.make_async_copy(near, near, near_sem).wait()

    def put_hidden(h, m):
        src = near.at[m, :, pl.ds(pl.multiple_of(h * slab, 128), slab)]
        put(src, rows.at[sp], row_sem.at[sp], {"sp": (2 * h + m) * 2 + y}, 2)

    own_rows = near.at[parity, :, pl.ds(pl.multiple_of(upper * slab, 128), slab)]
    put(own_rows, rows.at[sp], row_sem.at[sp], across, 6)
    pl.when(follows)(lambda: put_hidden(upper, 1 - parity))
    pltpu.make_async_copy(own_rows, rows.at[sp], row_sem.at[sp]).start()
    next_round(0)
    put_weights(away_head, leads, 1)
    pl.when(leads)(lambda: put_hidden(upper, 1 - parity))
    first_far = jnp.where(inner & leads, 1 - upper, upper)
    put_hidden(1 - upper, first_far)
    for index, (src, dst) in enumerate(small):
        pltpu.make_async_copy(src, dst, raw_sem.at[index]).wait()
    square = (
        lax.broadcasted_iota(jnp.int32, (tokens, 128), 0)
        == lax.broadcasted_iota(jnp.int32, (tokens, 128), 1)
    )
    for m in range(2):
        gain_send[m] = (gain_raw0, gain_raw1)[m][...].astype(jnp.float32).reshape(1, -1)
        wide_row = near[m].astype(jnp.float32)
        inverse = lax.rsqrt(jnp.mean(wide_row * wide_row, axis=-1, keepdims=True) + EPS)
        row_send[m] = jnp.sum(jnp.where(square, inverse, 0.0), axis=0, keepdims=True)
        row_send[m, :, 64:64 + tokens] = doc_raw[m].astype(jnp.float32)
    next_round(1)
    put_hidden(1 - upper, 1 - first_far)
    for m in range(2):
        for yy in range(2):
            for cc in range(2):
                send(
                    gain_send.at[m], gain_rows.at[mine], gain_sem,
                    {"sp": (upper * 2 + m) * 2 + yy, "fsdp": cc}, 3, (parity == m) & (y == yy) & (core == cc),
                )
    next_round(2)
    token_rows = pl.ds(pl.multiple_of(sp * tokens, 16), tokens)
    for m in range(2):
        for yy in range(2):
            for h in range(2):
                to_sp = (2 * h + m) * 2 + yy
                send(row_send.at[m], row_data.at[sp], data_sem.at[upper], {"sp": to_sp}, 4, sp == to_sp)
    pl.when(inner)(lambda: put_weights(home_head, leads, 2))
    for m in range(2):
        for yy in range(2):
            for h in range(2):
                to_sp, head = (2 * h + m) * 2 + yy, yy * 2 + h
                send(
                    queries[m].at[0, :, head * head_cols:(head + 1) * head_cols],
                    query_rows.at[token_rows], query_sem.at[upper], {"sp": to_sp}, 5, sp == to_sp,
                )
    pl.when(jnp.logical_not(inner))(lambda: put_weights(home_head, leads, 2))

    def pass_rows(step):
        from_z = order[step]
        block = from_z * 2 + y
        arrive(rows.at[block], row_sem.at[block], f"whid{step}")
        put(rows.at[block], rows.at[block], row_sem.at[block], across, 6)

    order = (z, near_z, 3 * (1 - upper), 2 - upper)
    def forward_all(b, onward, *lanes):
        for zz, yy in lanes:
            forward(b, zz, yy, onward)

    side_lane, next_lane, last_lane = (parity, 1 - y), (1 - parity, y), (1 - parity, 1 - y)

    def led(b, lead, *lanes):
        pl.when(lead)(lambda: forward_all(b, True, *lanes))

    def followed(b, lead, *lanes):
        pl.when(jnp.logical_not(lead))(lambda: forward_all(b, False, *lanes))

    arrive(rows.at[sp], row_sem.at[sp], "whid0")
    led(away_head, leads, side_lane, next_lane)
    pass_rows(1)
    led(away_head, leads, last_lane)
    pl.when(follows)(lambda: pass_rows(2))
    followed(away_head, leads, side_lane, next_lane)
    pl.when(leads)(lambda: pass_rows(2))
    pass_rows(3)
    followed(away_head, leads, last_lane)
    led(home_head, leads, side_lane, next_lane)
    arrive(gain_rows, gain_sem, "wgain")
    arrive_own(away_head)
    arrive_side(away_head)
    gain_row = jnp.concatenate([gain_rows[s] for s in range(8)], axis=1)
    partner = {"sp": far_z * 2 + y}

    def block_of(half, side, k):
        return half * 4 + 2 * k + (y if side == 0 else 1 - y)

    def project(half, side):
        for k in range(2):
            s = block_of(half, side, k)
            scale = jnp.sum(jnp.where(square, row_data[s], 0.0), axis=1, keepdims=True)
            spot = (side * 2 + k) * tokens
            normed[half, spot:spot + tokens, :] = (
                rows[s].astype(jnp.float32) * scale * gain_row
            ).astype(jnp.bfloat16)
        spot = side * 2 * tokens
        part = jnp.dot(
            normed[half, spot:spot + 2 * tokens, :], wide[away_head], preferred_element_type=jnp.float32
        )
        index = half * 2 + side
        key_send[index] = part[:, :HEAD_DIM]
        value_send[index] = part[:, HEAD_DIM:].astype(jnp.bfloat16)
        put(key_send.at[index], key_parts.at[index], part_sem.at[half], partner, 7)
        put(value_send.at[index], value_parts.at[index], value_sem.at[half], partner, 8)

    def arrive_data(half):
        arrive(row_data.at[pl.ds(4 * half, 4)], data_sem.at[half], "wdata")

    def arrive_rows(half):
        for k in range(2):
            block = block_of(half, 1, k)
            arrive(rows.at[block], row_sem.at[block], "wfwd")

    arrive_data(upper)
    project(upper, 0)
    arrive_rows(upper)
    project(upper, 1)
    led(home_head, leads, last_lane)
    arrive_data(1 - upper)
    project(1 - upper, 0)
    shifted = (
        lax.broadcasted_iota(jnp.int32, (tokens, 128), 0) + 64
        == lax.broadcasted_iota(jnp.int32, (tokens, 128), 1)
    )
    for s in range(8):
        column = jnp.sum(jnp.where(shifted, row_data[s], 0.0), axis=1, keepdims=True)
        doc_wide[s * tokens:(s + 1) * tokens, :] = jnp.broadcast_to(column, (tokens, 128))
    query_index = lax.broadcasted_iota(jnp.int32, (length, length), 0)
    key_index = lax.broadcasted_iota(jnp.int32, (length, length), 1)
    doc_column = doc_wide[:, :1]
    doc_row = jnp.sum(jnp.where(query_index == key_index, doc_column, 0.0), axis=0, keepdims=True)
    followed(home_head, leads, side_lane, next_lane)
    arrive_rows(1 - upper)
    project(1 - upper, 1)
    followed(home_head, leads, last_lane)
    arrive(tables, table_sem, "wtable")
    arrive_own(home_head)

    def home_part(half, c):
        total = None
        for index in range(4):
            at = place_rows(index * 2 + c)
            part = jnp.dot(normed[half, :, at], wide[home_head, at, :], preferred_element_type=jnp.float32)
            total = part if total is None else total + part
        return total

    for half in range(2):
        home[half] = home_part(half, core)
    arrive_side(home_head)

    factor = HEAD_DIM ** (-0.5)
    head = y * 2 + upper
    out_columns = pl.ds(pl.multiple_of(head * head_cols, 128), head_cols)
    half_rows = length // 2

    def put_out(half):
        for k in range(4):
            to_sp = half * 4 + k
            send(
                mixed.at[half, k * tokens:(k + 1) * tokens], out.at[parity, 0, :, out_columns], out_sem,
                {"sp": to_sp}, 9, sp == to_sp,
            )

    for half in range(2):
        whole = home[half] + home_part(half, 1 - core)
        arrive(key_parts.at[2 * half:2 * half + 2], part_sem.at[half], f"wpart{half}")
        arrive(value_parts.at[2 * half:2 * half + 2], value_sem.at[half], f"wpart{half}")
        if half:
            pl.when(upper == 1)(lambda: put_out(0))
        for index in range(2 * half, 2 * half + 2):
            for k in range(2):
                block = pl.ds(pl.multiple_of(block_of(half, index % 2, k) * tokens, 16), tokens)
                near_rows = slice(k * tokens, (k + 1) * tokens)
                spot = (index % 2 * 2 + k) * tokens
                raw_keys = whole[spot:spot + tokens, :HEAD_DIM] + key_parts[index, near_rows, :]
                raw_values = whole[spot:spot + tokens, HEAD_DIM:] + value_parts[index, near_rows, :].astype(jnp.float32)
                key_heads[block, :] = (
                    raw_keys * tables[0, block, :] + pltpu.roll(raw_keys, HEAD_DIM // 2, 1) * tables[1, block, :]
                ).astype(jnp.bfloat16)
                value_heads[block, :] = raw_values.astype(jnp.bfloat16)
        first, last = half * half_rows, (half + 1) * half_rows
        arrive(query_rows.at[first:last], query_sem.at[half], f"wq{half}")
        allowed = (
            lax.broadcasted_iota(jnp.int32, (half_rows, last), 1)
            <= first + lax.broadcasted_iota(jnp.int32, (half_rows, last), 0)
        ) & (doc_row[:, :last] == doc_wide[first:last, :1])
        stacked = jnp.concatenate(
            [query_rows[first:last, g * HEAD_DIM:(g + 1) * HEAD_DIM] for g in range(group_size)], axis=0
        )
        scores = lax.dot_general(
            stacked, key_heads[:last, :], (((1,), (1,)), ((), ())), preferred_element_type=jnp.float32
        ) * factor
        scores = jnp.where(jnp.concatenate([allowed] * group_size, axis=0), scores, MASKED)
        highest = jnp.max(scores, axis=-1, keepdims=True)
        exponent = jnp.exp(scores - highest)
        weights = (exponent / jnp.sum(exponent, axis=-1, keepdims=True)).astype(jnp.bfloat16)
        blended = jnp.dot(weights, value_heads[:last, :], preferred_element_type=jnp.float32).astype(jnp.bfloat16)
        for g in range(group_size):
            mixed[half, :, g * HEAD_DIM:(g + 1) * HEAD_DIM] = blended[g * half_rows:(g + 1) * half_rows, :]
        if half:
            put_out(1)
        else:
            pl.when(upper == 0)(lambda: put_out(0))

    def sent(ref, index):
        pltpu.make_async_copy(ref, ref, send_sem.at[index]).wait()

    with scope("wsend"):
        sent(wide.at[0], 0)


        @pl.when(leads)
        def _():
            sent(wide.at[:, :6 * features], 1)

        sent(rows.at[:3], 2)
        sent(gain_rows.at[:7], 3)
        sent(row_data.at[:7], 4)
        sent(query_rows.at[:7 * tokens], 5)
        sent(rows.at[:4], 6)
        sent(key_send, 7)
        sent(value_send, 8)
        sent(query_rows.at[:7 * tokens], 9)
    arrive(out, out_sem, "wout")


def fused(mesh, hiddens, queries, documents, gains, keys, values):
    sp = mesh.shape["sp"]
    tokens, features = hiddens[0].shape[1], keys[0].shape[0]
    kv_heads = keys[0].shape[1] // HEAD_DIM
    head_cols = queries[0].shape[2] // kv_heads
    length = sp * tokens
    half_dim = HEAD_DIM // 2
    frequency = ROPE_BASE ** (-2.0 * np.arange(half_dim) / HEAD_DIM)
    angles = np.arange(length)[:, None] * frequency[None, :]
    cosines = np.concatenate([np.cos(angles), np.cos(angles)], axis=1).astype(np.float32)
    sines = np.concatenate([-np.sin(angles), np.sin(angles)], axis=1).astype(np.float32)
    dma = pltpu.SemaphoreType.DMA
    bf16, f32 = jnp.bfloat16, jnp.float32
    out = pl.pallas_call(
        fused_kernel,
        out_shape=pltpu.VMEM((2, 1, tokens, queries[0].shape[2]), bf16),
        in_specs=[pl.BlockSpec(memory_space=pl.ANY)] * 13,
        out_specs=pl.BlockSpec(memory_space=pltpu.VMEM),
        scratch_shapes=[
            pltpu.VMEM((features,), bf16),
            pltpu.VMEM((features,), bf16),
            pltpu.VMEM((2, 1, tokens), jnp.int32),
            pltpu.VMEM((2,) + hiddens[0].shape[1:], bf16),
            pltpu.VMEM((sp, tokens, 8 * features), bf16),
            pltpu.VMEM((2, 8 * features, 2 * HEAD_DIM), bf16),
            pltpu.VMEM((2, 4 * tokens, 8 * features), bf16),
            pltpu.VMEM((2, 1, features), f32),
            pltpu.VMEM((8, 1, features), f32),
            pltpu.VMEM((2, 1, 128), f32),
            pltpu.VMEM((sp, 1, 128), f32),
            pltpu.VMEM((length, head_cols), bf16),
            pltpu.VMEM((length, 128), f32),
            pltpu.VMEM((4, 2 * tokens, HEAD_DIM), f32),
            pltpu.VMEM((4, 2 * tokens, HEAD_DIM), bf16),
            pltpu.VMEM((4, 2 * tokens, HEAD_DIM), f32),
            pltpu.VMEM((4, 2 * tokens, HEAD_DIM), bf16),
            pltpu.VMEM((2, length // 2, 2 * HEAD_DIM), f32),
            pltpu.VMEM((length, HEAD_DIM), bf16),
            pltpu.VMEM((length, HEAD_DIM), bf16),
            pltpu.VMEM((2, length // 2, head_cols), bf16),
            pltpu.VMEM((2, length, HEAD_DIM), f32),
            pltpu.SemaphoreType.REGULAR((3,)),
            dma((4,)),
            dma(()),
            dma(()),
            dma((10,)),
            dma((sp,)),
            dma((2, 4)),
            dma((2,)),
            dma(()),
            dma((2,)),
            dma((2,)),
            dma((2,)),
            dma((2,)),
            dma(()),
        ],
        compiler_params=pltpu.CompilerParams(collective_id=0, has_side_effects=True),
        name="fused",
    )(
        *hiddens, *queries, *keys, *values, np.stack([cosines, sines]),
        *gains, *documents,
    )
    return out[0], out[1]


def per_device(
    mesh,
    policy_hidden,
    policy_queries,
    policy_documents,
    policy_gain,
    policy_key_weight,
    policy_value_weight,
    frozen_hidden,
    frozen_queries,
    frozen_documents,
    frozen_gain,
    frozen_key_weight,
    frozen_value_weight,
):
    if fits(mesh, policy_hidden, policy_queries, policy_key_weight):
        return fused(
            mesh,
            (policy_hidden, frozen_hidden),
            (policy_queries, frozen_queries),
            (policy_documents, frozen_documents),
            (policy_gain, frozen_gain),
            (policy_key_weight, frozen_key_weight),
            (policy_value_weight, frozen_value_weight),
        )
    policy_mixed = run_model(
        policy_hidden,
        policy_queries,
        policy_documents,
        policy_gain,
        policy_key_weight,
        policy_value_weight,
    )
    frozen_mixed = run_model(
        frozen_hidden,
        frozen_queries,
        frozen_documents,
        frozen_gain,
        frozen_key_weight,
        frozen_value_weight,
    )
    return (policy_mixed, frozen_mixed)


def solution(mesh):
    return jax.shard_map(
        functools.partial(per_device, mesh),
        mesh=mesh,
        in_specs=(
            P(("groups", "fsdp"), "sp", None),
            P(("groups", "fsdp"), "sp", None),
            P(("groups", "fsdp"), "sp"),
            P(("sp", "fsdp")),
            P(("sp", "fsdp"), None),
            P(("sp", "fsdp"), None),
            P(("groups", "fsdp"), "sp", None),
            P(("groups", "fsdp"), "sp", None),
            P(("groups", "fsdp"), "sp"),
            P(("sp", "fsdp")),
            P(("sp", "fsdp"), None),
            P(("sp", "fsdp"), None),
        ),
        out_specs=(P(("groups", "fsdp"), "sp", None), P(("groups", "fsdp"), "sp", None)),
        check_vma=False,
    )
```

```python
import contextlib
import functools

import jax
import jax.numpy as jnp
import numpy as np
from jax import lax
from jax.experimental import pallas as pl
from jax.experimental.pallas import tpu as pltpu
from jax.sharding import PartitionSpec as P

HEAD_DIM = 128


EPS = 1e-05
ROPE_BASE = 500000.0
MASKED = -1e30


def rotate(raw_keys, positions):
    half_dim = HEAD_DIM // 2
    frequency = jnp.exp(
        -jnp.log(ROPE_BASE) * jnp.arange(half_dim, dtype=jnp.float32) * 2.0 / HEAD_DIM
    )
    angles = positions.astype(jnp.float32)[:, None] * frequency[None, :]
    cosines = jnp.cos(angles)[:, None, :]
    sines = jnp.sin(angles)[:, None, :]
    front_half = raw_keys[..., :half_dim]
    back_half = raw_keys[..., half_dim:]
    return jnp.concatenate(
        [front_half * cosines - back_half * sines, back_half * cosines + front_half * sines],
        axis=-1,
    )


def project(hidden, gain, key_weight, value_weight):
    tokens = hidden.shape[1]
    widened = hidden[0].astype(jnp.float32)
    inverse = lax.rsqrt(jnp.mean(widened * widened, axis=-1, keepdims=True) + EPS)
    scaled = widened * inverse
    gain_rows = lax.all_gather(gain, ("sp", "fsdp"), axis=0, tiled=True)
    key_rows = lax.all_gather(key_weight, ("sp", "fsdp"), axis=0, tiled=True)
    value_rows = lax.all_gather(value_weight, ("sp", "fsdp"), axis=0, tiled=True)
    normed = (scaled * gain_rows.astype(jnp.float32)[None, :]).astype(jnp.bfloat16)
    raw_keys = jnp.dot(normed, key_rows, preferred_element_type=jnp.float32)
    raw_values = jnp.dot(normed, value_rows, preferred_element_type=jnp.float32)
    positions = lax.axis_index("sp") * tokens + jnp.arange(tokens, dtype=jnp.int32)
    key_heads = rotate(raw_keys.reshape(tokens, -1, HEAD_DIM), positions).astype(jnp.bfloat16)
    value_heads = raw_values.astype(jnp.bfloat16).reshape(tokens, -1, HEAD_DIM)
    return (key_heads, value_heads)


def attend(queries, key_heads, value_heads, documents):
    length = queries.shape[0]
    head_count = queries.shape[1]
    block_rows = min(512, length)
    margin = min(512, length // 2)
    window = block_rows + margin
    factor = HEAD_DIM ** (-0.5)
    offsets = jnp.arange(block_rows, dtype=jnp.int32)
    window_offsets = jnp.arange(window, dtype=jnp.int32)
    padding = jnp.zeros((margin, head_count, HEAD_DIM), jnp.bfloat16)
    padded_keys = jnp.concatenate([padding, key_heads], axis=0)
    padded_values = jnp.concatenate([padding, value_heads], axis=0)
    padded_docs = jnp.concatenate([jnp.full((margin,), -1, jnp.int32), documents], axis=0)

    def one_block(block_index):
        first = block_index * block_rows
        query_block = lax.dynamic_slice_in_dim(queries, first, block_rows, 0)
        query_docs = lax.dynamic_slice_in_dim(documents, first, block_rows, 0)
        query_positions = first + offsets
        key_block = lax.dynamic_slice_in_dim(padded_keys, first, window, 0)
        value_block = lax.dynamic_slice_in_dim(padded_values, first, window, 0)
        key_docs = lax.dynamic_slice_in_dim(padded_docs, first, window, 0)
        key_positions = first - margin + window_offsets
        allowed = (key_positions[None, :] <= query_positions[:, None]) & (
            key_docs[None, :] == query_docs[:, None]
        )
        scores = (
            jnp.einsum("qnd,knd->nqk", query_block, key_block, preferred_element_type=jnp.float32)
            * factor
        )
        scores = jnp.where(allowed[None], scores, MASKED)
        highest = jnp.max(scores, axis=-1, keepdims=True)
        exponent = jnp.where(allowed[None], jnp.exp(scores - highest), 0.0)
        weights = (exponent / jnp.sum(exponent, axis=-1, keepdims=True)).astype(jnp.bfloat16)
        blended = jnp.einsum(
            "nqk,knd->qnd", weights, value_block, preferred_element_type=jnp.float32
        )
        return blended.astype(jnp.bfloat16)

    blocks = lax.map(one_block, jnp.arange(length // block_rows, dtype=jnp.int32))
    return blocks.reshape(length, head_count, HEAD_DIM)


def run_model(hidden, queries, documents, gain, key_weight, value_weight):
    tokens = hidden.shape[1]
    head_count = queries.shape[2] // HEAD_DIM
    query_local = queries[0].reshape(tokens, head_count, HEAD_DIM)
    every_doc = lax.all_gather(documents[0], "sp", axis=0, tiled=True)
    key_heads, value_heads = project(hidden, gain, key_weight, value_weight)
    group_size = head_count // key_heads.shape[1]
    wide_keys = jnp.repeat(key_heads, group_size, axis=1)
    wide_values = jnp.repeat(value_heads, group_size, axis=1)
    query_spread, key_spread, value_spread = (
        lax.all_to_all(query_local, "sp", split_axis=1, concat_axis=0, tiled=True),
        lax.all_to_all(wide_keys, "sp", split_axis=1, concat_axis=0, tiled=True),
        lax.all_to_all(wide_values, "sp", split_axis=1, concat_axis=0, tiled=True),
    )
    mixed = attend(query_spread, key_spread, value_spread, every_doc)
    returned = lax.all_to_all(mixed, "sp", split_axis=0, concat_axis=1, tiled=True)
    return returned.reshape(1, tokens, head_count * HEAD_DIM)


MESH = pl.DeviceIdType.MESH
TRACE = False


def fits(mesh, hidden, queries, key_weight):
    sp, cores = mesh.shape["sp"], mesh.shape["fsdp"]
    tokens = hidden.shape[1]
    kv_heads = key_weight.shape[1] // HEAD_DIM
    return (
        cores == 2
        and mesh.shape["groups"] == 2
        and sp == 8
        and kv_heads == 4
        and queries.shape[2] % (kv_heads * HEAD_DIM) == 0
        and key_weight.shape[0] % 128 == 0
        and hidden.shape[2] == key_weight.shape[0] * sp * cores
        and tokens % 16 == 0
        and tokens <= 64
    )


def fused_kernel(
    hidden0, hidden1, queries0, queries1, key0, key1, value0, value1, table,
    gain0, gain1, documents0, documents1,
    out,
    gain_raw0, gain_raw1, doc_raw, near, rows, wide, normed, gain_send, gain_rows, row_send, row_data, query_rows, doc_wide,
    key_send, value_send, key_parts, value_parts, bias, home, key_heads, value_heads, mixed, tables,
    ready, raw_sem, near_sem, table_sem, send_sem, row_sem, wide_sem, side_sem, gain_sem, data_sem, query_sem, part_sem, value_sem, out_sem,
):
    hiddens, queries = (hidden0, hidden1), (queries0, queries1)
    keys, values = (key0, key1), (value0, value1)
    tokens, features = hidden0.shape[1], key0.shape[0]
    slab = 8 * features
    head_cols = query_rows.shape[1]
    group_size = head_cols // HEAD_DIM
    length = query_rows.shape[0]
    sp, core, plane = lax.axis_index("sp"), lax.axis_index("fsdp"), lax.axis_index("groups")
    z, y = sp // 2, sp % 2
    upper, parity = z // 2, z % 2
    near_z = z + 1 - 2 * parity
    far_z = lax.rem(z + 2, 4)

    def scope(name):
        return jax.named_scope(name) if TRACE else contextlib.nullcontext()

    inner = upper != parity
    greeted = 4 + jnp.where(inner, 1, 0)

    def greet(semaphore):
        for target in (
            {"sp": near_z * 2 + y}, {"sp": z * 2 + 1 - y}, {"groups": 1 - plane}, {"fsdp": 1 - core},
        ):
            pl.semaphore_signal(semaphore, inc=1, device_id=target, device_id_type=MESH)

        @pl.when(inner)
        def _():
            pl.semaphore_signal(semaphore, inc=1, device_id={"sp": (3 - z) * 2 + y}, device_id_type=MESH)

    barrier = pltpu.get_barrier_semaphore()
    greet(barrier)

    def place(zz, yy, cc):
        return (zz * 2 + yy) * 2 + cc

    def place_rows(index):
        return pl.ds(pl.multiple_of(index * features, 128), features)

    mine = place(parity, y, core)
    leads, follows = core == plane, core != plane

    def columns(half, b):
        return pl.ds(pl.multiple_of((half * 2 + b) * HEAD_DIM, HEAD_DIM), HEAD_DIM)

    for m in range(2):
        pltpu.make_async_copy(hiddens[m].at[0], near.at[m], near_sem).start()
    small = (
        (gain0, gain_raw0), (gain1, gain_raw1), (documents0, doc_raw.at[0]), (documents1, doc_raw.at[1]),
    )
    for index, (src, dst) in enumerate(small):
        pltpu.make_async_copy(src, dst, raw_sem.at[index]).start()
    with scope("wbar"):
        pl.semaphore_wait(barrier, greeted)
    greet(ready.at[0])

    def next_round(step):
        with scope(f"wround{step}"):
            pl.semaphore_wait(ready.at[step], greeted)
        if step < 2:
            greet(ready.at[step + 1])

    def put(src, dst, recv, target, sent, away=None):
        def start():
            pltpu.make_async_remote_copy(
                src_ref=src, dst_ref=dst, send_sem=send_sem.at[sent], recv_sem=recv,
                device_id=target, device_id_type=MESH,
            ).start()

        if away is None:
            start()
        else:
            pl.when(away)(start)

    def send(src, dst, recv, target, sent, own):
        put(src, dst, recv, target, sent, jnp.logical_not(own))

        @pl.when(own)
        def _():
            pltpu.make_async_copy(src, dst, recv).start()

    def put_weight(b, half, target, sent, recv, model, when=None):
        for index, weights in enumerate((keys, values)):
            cols = slice(index * HEAD_DIM, (index + 1) * HEAD_DIM)
            for m in range(2):
                put(
                    weights[m].at[:, columns(half, b)], wide.at[b, place_rows(mine), cols], recv,
                    target, sent, model == m if when is None else (model == m) & when,
                )

    def arrive(dst, recv, name):
        with scope(name):
            pltpu.make_async_copy(dst, dst, recv).wait()

    def lane(zz, yy):
        return zz * 2 + yy

    def forward(b, zz, yy, onward):
        block = wide.at[b, place_rows(place(zz, yy, core))]
        arrive(block, wide_sem.at[b, lane(zz, yy)], ("wa" if b is away_head else "wh") + f"{1 if zz is parity else 0}{1 if yy is y else 0}")
        if onward:
            put(block, block, wide_sem.at[b, lane(zz, yy)], {"groups": 1 - plane}, 1)
        put(block, block, side_sem.at[b], beside, 0)

    def arrive_own(b):
        arrive(wide.at[b, place_rows(mine)], wide_sem.at[b, lane(parity, y)], "wown")

    def arrive_side(b):
        arrive(wide.at[b, :4 * features], side_sem.at[b], "wside")

    across, beside, along = {"sp": z * 2 + 1 - y}, {"fsdp": 1 - core}, {"sp": near_z * 2 + y}
    beyond = {"sp": near_z * 2 + 1 - y}
    away_head, home_head = 1 - upper, upper

    own_lane = lane(parity, y)

    def put_weights(b, lead, first):
        recv = wide_sem.at[b, own_lane]
        if first != 1:
            put_weight(b, 1 - y, across, 1, recv, parity, lead)
            put_weight(b, y, along, 1, recv, 1 - parity, lead)
            put_weight(b, y, beside, 0, side_sem.at[b], parity)
        if first != 0:
            put_weight(b, 1 - y, beyond, 1, recv, 1 - parity, lead)

    put_weights(away_head, leads, 0)
    for m in range(2):
        @pl.when(parity == m)
        def _(m=m):
            for b in range(2):
                target = wide.at[b, place_rows(mine)]
                pltpu.make_async_copy(
                    keys[m].at[:, columns(y, b)], target.at[:, :HEAD_DIM], wide_sem.at[b, own_lane]
                ).start()
                pltpu.make_async_copy(
                    values[m].at[:, columns(y, b)], target.at[:, HEAD_DIM:], wide_sem.at[b, own_lane]
                ).start()

    pltpu.make_async_copy(table, tables, table_sem).start()
    pltpu.make_async_copy(near, near, near_sem).wait()

    def put_hidden(h, m):
        src = near.at[m, :, pl.ds(pl.multiple_of(h * slab, 128), slab)]
        put(src, rows.at[sp], row_sem.at[sp], {"sp": (2 * h + m) * 2 + y}, 2)

    own_rows = near.at[parity, :, pl.ds(pl.multiple_of(upper * slab, 128), slab)]
    put(own_rows, rows.at[sp], row_sem.at[sp], across, 6)
    pl.when(follows)(lambda: put_hidden(upper, 1 - parity))
    pltpu.make_async_copy(own_rows, rows.at[sp], row_sem.at[sp]).start()
    next_round(0)
    put_weights(away_head, leads, 1)
    pl.when(leads)(lambda: put_hidden(upper, 1 - parity))
    first_far = jnp.where(inner & leads, 1 - upper, upper)
    put_hidden(1 - upper, first_far)
    for index, (src, dst) in enumerate(small):
        pltpu.make_async_copy(src, dst, raw_sem.at[index]).wait()
    square = (
        lax.broadcasted_iota(jnp.int32, (tokens, 128), 0)
        == lax.broadcasted_iota(jnp.int32, (tokens, 128), 1)
    )
    for m in range(2):
        gain_send[m] = (gain_raw0, gain_raw1)[m][...].astype(jnp.float32).reshape(1, -1)
        wide_row = near[m].astype(jnp.float32)
        inverse = lax.rsqrt(jnp.mean(wide_row * wide_row, axis=-1, keepdims=True) + EPS)
        row_send[m] = jnp.sum(jnp.where(square, inverse, 0.0), axis=0, keepdims=True)
        row_send[m, :, 64:64 + tokens] = doc_raw[m].astype(jnp.float32)
    next_round(1)
    put_hidden(1 - upper, 1 - first_far)
    for m in range(2):
        for yy in range(2):
            for cc in range(2):
                send(
                    gain_send.at[m], gain_rows.at[mine], gain_sem,
                    {"sp": (upper * 2 + m) * 2 + yy, "fsdp": cc}, 3, (parity == m) & (y == yy) & (core == cc),
                )
    next_round(2)
    token_rows = pl.ds(pl.multiple_of(sp * tokens, 16), tokens)
    for m in range(2):
        for yy in range(2):
            for h in range(2):
                to_sp = (2 * h + m) * 2 + yy
                send(row_send.at[m], row_data.at[sp], data_sem.at[upper], {"sp": to_sp}, 4, sp == to_sp)
    pl.when(inner)(lambda: put_weights(home_head, leads, 2))
    for m in range(2):
        for yy in range(2):
            for h in range(2):
                to_sp, head = (2 * h + m) * 2 + yy, yy * 2 + h
                send(
                    queries[m].at[0, :, head * head_cols:(head + 1) * head_cols],
                    query_rows.at[token_rows], query_sem.at[upper], {"sp": to_sp}, 5, sp == to_sp,
                )
    pl.when(jnp.logical_not(inner))(lambda: put_weights(home_head, leads, 2))

    def pass_rows(step):
        from_z = order[step]
        block = from_z * 2 + y
        arrive(rows.at[block], row_sem.at[block], f"whid{step}")
        put(rows.at[block], rows.at[block], row_sem.at[block], across, 6)

    order = (z, near_z, 3 * (1 - upper), 2 - upper)
    def forward_all(b, onward, *lanes):
        for zz, yy in lanes:
            forward(b, zz, yy, onward)

    side_lane, next_lane, last_lane = (parity, 1 - y), (1 - parity, y), (1 - parity, 1 - y)

    def led(b, lead, *lanes):
        pl.when(lead)(lambda: forward_all(b, True, *lanes))

    def followed(b, lead, *lanes):
        pl.when(jnp.logical_not(lead))(lambda: forward_all(b, False, *lanes))

    arrive(rows.at[sp], row_sem.at[sp], "whid0")
    led(away_head, leads, side_lane, next_lane)
    pass_rows(1)
    led(away_head, leads, last_lane)
    pl.when(follows)(lambda: pass_rows(2))
    followed(away_head, leads, side_lane, next_lane)
    pl.when(leads)(lambda: pass_rows(2))
    pass_rows(3)
    followed(away_head, leads, last_lane)
    led(home_head, leads, side_lane, next_lane)
    arrive(gain_rows, gain_sem, "wgain")
    arrive_own(away_head)
    arrive_side(away_head)
    gain_row = jnp.concatenate([gain_rows[s] for s in range(8)], axis=1)
    partner = {"sp": far_z * 2 + y}

    def block_of(half, side, k):
        return half * 4 + 2 * k + (y if side == 0 else 1 - y)

    def project(half, side):
        for k in range(2):
            s = block_of(half, side, k)
            scale = jnp.sum(jnp.where(square, row_data[s], 0.0), axis=1, keepdims=True)
            spot = (side * 2 + k) * tokens
            normed[half, spot:spot + tokens, :] = (
                rows[s].astype(jnp.float32) * scale * gain_row
            ).astype(jnp.bfloat16)
        spot = side * 2 * tokens
        part = jnp.dot(
            normed[half, spot:spot + 2 * tokens, :], wide[away_head], preferred_element_type=jnp.float32
        )
        index = half * 2 + side
        key_send[index] = part[:, :HEAD_DIM]
        value_send[index] = part[:, HEAD_DIM:].astype(jnp.bfloat16)
        put(key_send.at[index], key_parts.at[index], part_sem.at[half], partner, 7)
        put(value_send.at[index], value_parts.at[index], value_sem.at[half], partner, 8)

    def arrive_data(half):
        arrive(row_data.at[pl.ds(4 * half, 4)], data_sem.at[half], "wdata")

    def arrive_rows(half):
        for k in range(2):
            block = block_of(half, 1, k)
            arrive(rows.at[block], row_sem.at[block], "wfwd")

    arrive_data(upper)
    project(upper, 0)
    arrive_rows(upper)
    project(upper, 1)
    led(home_head, leads, last_lane)
    arrive_data(1 - upper)
    project(1 - upper, 0)
    shifted = (
        lax.broadcasted_iota(jnp.int32, (tokens, 128), 0) + 64
        == lax.broadcasted_iota(jnp.int32, (tokens, 128), 1)
    )
    for s in range(8):
        column = jnp.sum(jnp.where(shifted, row_data[s], 0.0), axis=1, keepdims=True)
        doc_wide[s * tokens:(s + 1) * tokens, :] = jnp.broadcast_to(column, (tokens, 128))
    query_index = lax.broadcasted_iota(jnp.int32, (length, length), 0)
    key_index = lax.broadcasted_iota(jnp.int32, (length, length), 1)
    doc_column = doc_wide[:, :1]
    doc_row = jnp.sum(jnp.where(query_index == key_index, doc_column, 0.0), axis=0, keepdims=True)
    bias[...] = jnp.where((key_index <= query_index) & (doc_row == doc_column), 0.0, MASKED)
    followed(home_head, leads, side_lane, next_lane)
    arrive_rows(1 - upper)
    project(1 - upper, 1)
    followed(home_head, leads, last_lane)
    arrive(tables, table_sem, "wtable")
    arrive_own(home_head)

    def home_part(half, c):
        total = None
        for index in range(4):
            at = place_rows(index * 2 + c)
            part = jnp.dot(normed[half, :, at], wide[home_head, at, :], preferred_element_type=jnp.float32)
            total = part if total is None else total + part
        return total

    for half in range(2):
        home[half] = home_part(half, core)
    arrive_side(home_head)

    factor = HEAD_DIM ** (-0.5)
    head = y * 2 + upper
    out_columns = pl.ds(pl.multiple_of(head * head_cols, 128), head_cols)
    half_rows = length // 2

    def put_out(half):
        for k in range(4):
            to_sp = half * 4 + k
            send(
                mixed.at[half, k * tokens:(k + 1) * tokens], out.at[parity, 0, :, out_columns], out_sem,
                {"sp": to_sp}, 9, sp == to_sp,
            )

    for half in range(2):
        whole = home[half] + home_part(half, 1 - core)
        arrive(key_parts.at[2 * half:2 * half + 2], part_sem.at[half], f"wpart{half}")
        arrive(value_parts.at[2 * half:2 * half + 2], value_sem.at[half], f"wpart{half}")
        if half:
            pl.when(z == 3)(lambda: put_out(0))
        for index in range(2 * half, 2 * half + 2):
            for k in range(2):
                block = pl.ds(pl.multiple_of(block_of(half, index % 2, k) * tokens, 16), tokens)
                near_rows = slice(k * tokens, (k + 1) * tokens)
                spot = (index % 2 * 2 + k) * tokens
                raw_keys = whole[spot:spot + tokens, :HEAD_DIM] + key_parts[index, near_rows, :]
                raw_values = whole[spot:spot + tokens, HEAD_DIM:] + value_parts[index, near_rows, :].astype(jnp.float32)
                key_heads[block, :] = (
                    raw_keys * tables[0, block, :] + pltpu.roll(raw_keys, HEAD_DIM // 2, 1) * tables[1, block, :]
                ).astype(jnp.bfloat16)
                value_heads[block, :] = raw_values.astype(jnp.bfloat16)
        first, last = half * half_rows, (half + 1) * half_rows
        arrive(query_rows.at[first:last], query_sem.at[half], f"wq{half}")
        stacked = jnp.concatenate(
            [query_rows[first:last, g * HEAD_DIM:(g + 1) * HEAD_DIM] for g in range(group_size)], axis=0
        )
        scores = lax.dot_general(
            stacked, key_heads[:last, :], (((1,), (1,)), ((), ())), preferred_element_type=jnp.float32
        ) * factor
        scores = scores + jnp.concatenate([bias[first:last, :last]] * group_size, axis=0)
        highest = jnp.max(scores, axis=-1, keepdims=True)
        exponent = jnp.exp(scores - highest)
        weights = (exponent / jnp.sum(exponent, axis=-1, keepdims=True)).astype(jnp.bfloat16)
        blended = jnp.dot(weights, value_heads[:last, :], preferred_element_type=jnp.float32).astype(jnp.bfloat16)
        for g in range(group_size):
            mixed[half, :, g * HEAD_DIM:(g + 1) * HEAD_DIM] = blended[g * half_rows:(g + 1) * half_rows, :]
        if half:
            put_out(1)
        else:
            pl.when(z < 3)(lambda: put_out(0))

    def sent(ref, index):
        pltpu.make_async_copy(ref, ref, send_sem.at[index]).wait()

    with scope("wsend"):
        sent(wide.at[0], 0)


        @pl.when(leads)
        def _():
            sent(wide.at[:, :6 * features], 1)

        sent(rows.at[:3], 2)
        sent(gain_rows.at[:7], 3)
        sent(row_data.at[:7], 4)
        sent(query_rows.at[:7 * tokens], 5)
        sent(rows.at[:4], 6)
        sent(key_send, 7)
        sent(value_send, 8)
        sent(query_rows.at[:7 * tokens], 9)
    arrive(out, out_sem, "wout")


def fused(mesh, hiddens, queries, documents, gains, keys, values):
    sp = mesh.shape["sp"]
    tokens, features = hiddens[0].shape[1], keys[0].shape[0]
    kv_heads = keys[0].shape[1] // HEAD_DIM
    head_cols = queries[0].shape[2] // kv_heads
    length = sp * tokens
    half_dim = HEAD_DIM // 2
    frequency = ROPE_BASE ** (-2.0 * np.arange(half_dim) / HEAD_DIM)
    angles = np.arange(length)[:, None] * frequency[None, :]
    cosines = np.concatenate([np.cos(angles), np.cos(angles)], axis=1).astype(np.float32)
    sines = np.concatenate([-np.sin(angles), np.sin(angles)], axis=1).astype(np.float32)
    dma = pltpu.SemaphoreType.DMA
    bf16, f32 = jnp.bfloat16, jnp.float32
    out = pl.pallas_call(
        fused_kernel,
        out_shape=pltpu.VMEM((2, 1, tokens, queries[0].shape[2]), bf16),
        in_specs=[pl.BlockSpec(memory_space=pl.ANY)] * 13,
        out_specs=pl.BlockSpec(memory_space=pltpu.VMEM),
        scratch_shapes=[
            pltpu.VMEM((features,), bf16),
            pltpu.VMEM((features,), bf16),
            pltpu.VMEM((2, 1, tokens), jnp.int32),
            pltpu.VMEM((2,) + hiddens[0].shape[1:], bf16),
            pltpu.VMEM((sp, tokens, 8 * features), bf16),
            pltpu.VMEM((2, 8 * features, 2 * HEAD_DIM), bf16),
            pltpu.VMEM((2, 4 * tokens, 8 * features), bf16),
            pltpu.VMEM((2, 1, features), f32),
            pltpu.VMEM((8, 1, features), f32),
            pltpu.VMEM((2, 1, 128), f32),
            pltpu.VMEM((sp, 1, 128), f32),
            pltpu.VMEM((length, head_cols), bf16),
            pltpu.VMEM((length, 128), f32),
            pltpu.VMEM((4, 2 * tokens, HEAD_DIM), f32),
            pltpu.VMEM((4, 2 * tokens, HEAD_DIM), bf16),
            pltpu.VMEM((4, 2 * tokens, HEAD_DIM), f32),
            pltpu.VMEM((4, 2 * tokens, HEAD_DIM), bf16),
            pltpu.VMEM((length, length), f32),
            pltpu.VMEM((2, length // 2, 2 * HEAD_DIM), f32),
            pltpu.VMEM((length, HEAD_DIM), bf16),
            pltpu.VMEM((length, HEAD_DIM), bf16),
            pltpu.VMEM((2, length // 2, head_cols), bf16),
            pltpu.VMEM((2, length, HEAD_DIM), f32),
            pltpu.SemaphoreType.REGULAR((3,)),
            dma((4,)),
            dma(()),
            dma(()),
            dma((10,)),
            dma((sp,)),
            dma((2, 4)),
            dma((2,)),
            dma(()),
            dma((2,)),
            dma((2,)),
            dma((2,)),
            dma((2,)),
            dma(()),
        ],
        compiler_params=pltpu.CompilerParams(collective_id=0, has_side_effects=True),
        name="fused",
    )(
        *hiddens, *queries, *keys, *values, np.stack([cosines, sines]),
        *gains, *documents,
    )
    return out[0], out[1]


def per_device(
    mesh,
    policy_hidden,
    policy_queries,
    policy_documents,
    policy_gain,
    policy_key_weight,
    policy_value_weight,
    frozen_hidden,
    frozen_queries,
    frozen_documents,
    frozen_gain,
    frozen_key_weight,
    frozen_value_weight,
):
    if fits(mesh, policy_hidden, policy_queries, policy_key_weight):
        return fused(
            mesh,
            (policy_hidden, frozen_hidden),
            (policy_queries, frozen_queries),
            (policy_documents, frozen_documents),
            (policy_gain, frozen_gain),
            (policy_key_weight, frozen_key_weight),
            (policy_value_weight, frozen_value_weight),
        )
    policy_mixed = run_model(
        policy_hidden,
        policy_queries,
        policy_documents,
        policy_gain,
        policy_key_weight,
        policy_value_weight,
    )
    frozen_mixed = run_model(
        frozen_hidden,
        frozen_queries,
        frozen_documents,
        frozen_gain,
        frozen_key_weight,
        frozen_value_weight,
    )
    return (policy_mixed, frozen_mixed)


def solution(mesh):
    return jax.shard_map(
        functools.partial(per_device, mesh),
        mesh=mesh,
        in_specs=(
            P(("groups", "fsdp"), "sp", None),
            P(("groups", "fsdp"), "sp", None),
            P(("groups", "fsdp"), "sp"),
            P(("sp", "fsdp")),
            P(("sp", "fsdp"), None),
            P(("sp", "fsdp"), None),
            P(("groups", "fsdp"), "sp", None),
            P(("groups", "fsdp"), "sp", None),
            P(("groups", "fsdp"), "sp"),
            P(("sp", "fsdp")),
            P(("sp", "fsdp"), None),
            P(("sp", "fsdp"), None),
        ),
        out_specs=(P(("groups", "fsdp"), "sp", None), P(("groups", "fsdp"), "sp", None)),
        check_vma=False,
    )
```
